16 devices in a mesh: dp: 4 (over z, y), tp: 4 (over x, core).
Axes of the slice: x: 2, y: 2, z: 2, core: 2. Of those that a mesh axis runs over, the one named last changes fastest.
Arguments:
- hidden: bfloat16 [64, 448, 2048], P('dp', 'tp'), parts along dimension 0
- prefix_len: int32 [64], P('dp'), parts along dimension 0
- valid_len: int32 [64], P('dp'), parts along dimension 0
- norm_attn: bfloat16 [2048], replicated
- w_query: bfloat16 [2048, 2048], P(None, 'tp')
- w_key: bfloat16 [2048, 256], replicated
- w_value: bfloat16 [2048, 256], replicated
- w_out: bfloat16 [2048, 2048], P('tp')
- norm_mlp: bfloat16 [2048], replicated
- w_gate: bfloat16 [2048, 16384], P(None, 'tp')
- w_up: bfloat16 [2048, 16384], P(None, 'tp')
- w_down: bfloat16 [16384, 2048], P('tp')
Outputs:
- output 1: bfloat16 [64, 448, 2048], P('dp', 'tp'), parts along dimension 0
- output 2: bfloat16 [64, 448, 256], P('dp', 'tp'), parts along dimension 0
- output 3: bfloat16 [64, 448, 256], P('dp', 'tp'), parts along dimension 0
There are 4 independent parts. The reference program is written for one: setup_inputs(seed, part) draws one part's arguments, and reference() takes and returns one part's arrays. A program takes and returns all parts, laid end to end along the dimension named above; an argument that names none is the same for every part.
All inputs are finite; a program needn't handle non-finite values.
Results may differ from the reference program's by a relative error of at most 0.0119926.
Values are sent between devices in bfloat16 or wider.
A program may use at most 1 GiB of HBM per device.

```python
import jax
import jax.numpy as jnp
from jax import lax

BATCH_SIZE = 16
IMG_TOKENS = 256
TEXT_TOKENS = 192
D_MODEL = 2048
NUM_HEADS = 8
HEAD_DIM = 256
FF_DIM = 16384

SEQ_LEN = IMG_TOKENS + TEXT_TOKENS
QUERY_WIDTH = NUM_HEADS * HEAD_DIM
QUERY_SCALE = HEAD_DIM ** -0.5
NORM_EPS = 1e-6
ROPE_BASE = 10000.0
MASK_FILL = -1e30


def setup_inputs(seed: int = 0, part: int = 0) -> dict:
    base_key = jax.random.key(seed)
    part_keys = jax.random.split(jax.random.fold_in(base_key, part), 4)
    weight_keys = jax.random.split(base_key, 10)
    noise_rows = jax.random.normal(part_keys[0], (BATCH_SIZE, SEQ_LEN, D_MODEL), jnp.float32)
    text_dir = jax.random.normal(part_keys[1], (BATCH_SIZE, 1, D_MODEL), jnp.float32)
    is_text = (jnp.arange(SEQ_LEN) >= IMG_TOKENS).astype(jnp.float32)[None, :, None]
    hidden = noise_rows + 2.0 * text_dir * is_text
    prompt_len = jax.random.randint(part_keys[2], (BATCH_SIZE,), 1, TEXT_TOKENS // 2 + 1)
    prefix_len = IMG_TOKENS + prompt_len
    valid_len = prefix_len + jax.random.randint(part_keys[3], (BATCH_SIZE,), 1, SEQ_LEN - prefix_len + 1)
    attn_gain = SEQ_LEN ** 0.5 / 6.0

    def draw_weight(key_index, shape, scale):
        return (jax.random.normal(weight_keys[key_index], shape, jnp.float32) * scale).astype(jnp.bfloat16)

    return {
        "hidden": hidden.astype(jnp.bfloat16),
        "prefix_len": prefix_len.astype(jnp.int32),
        "valid_len": valid_len.astype(jnp.int32),
        "norm_attn": draw_weight(0, (D_MODEL,), 0.3),
        "w_query": draw_weight(1, (D_MODEL, QUERY_WIDTH), 1.5 * D_MODEL ** -0.5),
        "w_key": draw_weight(2, (D_MODEL, HEAD_DIM), D_MODEL ** -0.5),
        "w_value": draw_weight(3, (D_MODEL, HEAD_DIM), D_MODEL ** -0.5),
        "w_out": draw_weight(4, (QUERY_WIDTH, D_MODEL), attn_gain * QUERY_WIDTH ** -0.5),
        "norm_mlp": draw_weight(5, (D_MODEL,), 0.3),
        "w_gate": draw_weight(6, (D_MODEL, FF_DIM), D_MODEL ** -0.5),
        "w_up": draw_weight(7, (D_MODEL, FF_DIM), D_MODEL ** -0.5),
        "w_down": draw_weight(8, (FF_DIM, D_MODEL), FF_DIM ** -0.5),
    }


def rms_norm(acts, norm_scale):
    acts_f32 = acts.astype(jnp.float32)
    inv_rms = lax.rsqrt(jnp.mean(acts_f32 * acts_f32, axis=-1, keepdims=True) + NORM_EPS)
    return (acts_f32 * inv_rms * (1.0 + norm_scale.astype(jnp.float32))).astype(jnp.bfloat16)


def rope_tables(positions):
    half_dim = HEAD_DIM // 2
    inv_freq = ROPE_BASE ** (-2.0 * jnp.arange(half_dim, dtype=jnp.float32) / HEAD_DIM)
    angles = positions.astype(jnp.float32)[:, None] * inv_freq[None, :]
    return jnp.cos(angles), jnp.sin(angles)


def apply_rope(vectors, cos_table, sin_table):
    half_dim = vectors.shape[-1] // 2
    first_half = vectors[..., :half_dim]
    second_half = vectors[..., half_dim:]
    return jnp.concatenate([first_half * cos_table - second_half * sin_table, second_half * cos_table + first_half * sin_table], axis=-1)


def reference(hidden, prefix_len, valid_len, norm_attn, w_query, w_key, w_value, w_out, norm_mlp, w_gate, w_up, w_down):
    positions = jnp.arange(SEQ_LEN)
    cos_table, sin_table = rope_tables(positions)
    row_pos = positions[:, None]
    col_pos = positions[None, :]

    def one_sample(sample_args):
        sample_rows, sample_prefix, sample_valid = sample_args
        normed = rms_norm(sample_rows, norm_attn)
        query_rows = jnp.dot(normed, w_query, preferred_element_type=jnp.float32).reshape(SEQ_LEN, NUM_HEADS, HEAD_DIM)
        query_rows = (apply_rope(query_rows, cos_table[:, None, :], sin_table[:, None, :]) * QUERY_SCALE).astype(jnp.bfloat16)
        key_rows = apply_rope(jnp.dot(normed, w_key, preferred_element_type=jnp.float32), cos_table, sin_table).astype(jnp.bfloat16)
        value_rows = jnp.dot(normed, w_value, preferred_element_type=jnp.float32).astype(jnp.bfloat16)
        allowed = (col_pos < sample_valid) & ((col_pos < sample_prefix) | (col_pos <= row_pos))

        def one_head(query_head):
            scores = jnp.dot(query_head, key_rows.T, preferred_element_type=jnp.float32)
            scores = jnp.where(allowed, scores, MASK_FILL)
            attn_probs = jax.nn.softmax(scores, axis=-1).astype(jnp.bfloat16)
            return jnp.dot(attn_probs, value_rows, preferred_element_type=jnp.float32).astype(jnp.bfloat16)

        attn_vals = lax.map(one_head, jnp.transpose(query_rows, (1, 0, 2)))
        attn_flat = jnp.transpose(attn_vals, (1, 0, 2)).reshape(SEQ_LEN, QUERY_WIDTH)
        attn_out = jnp.dot(attn_flat, w_out, preferred_element_type=jnp.float32).astype(jnp.bfloat16)
        hidden_mid = (sample_rows.astype(jnp.float32) + attn_out.astype(jnp.float32)).astype(jnp.bfloat16)
        normed_mlp = rms_norm(hidden_mid, norm_mlp)
        gate_proj = jnp.dot(normed_mlp, w_gate, preferred_element_type=jnp.float32)
        up_proj = jnp.dot(normed_mlp, w_up, preferred_element_type=jnp.float32)
        mlp_act = (jax.nn.gelu(gate_proj, approximate=True) * up_proj).astype(jnp.bfloat16)
        mlp_out = jnp.dot(mlp_act, w_down, preferred_element_type=jnp.float32).astype(jnp.bfloat16)
        hidden_out = (hidden_mid.astype(jnp.float32) + mlp_out.astype(jnp.float32)).astype(jnp.bfloat16)
        return hidden_out, key_rows, value_rows

    hidden_out, key_cache, value_cache = lax.map(one_sample, (hidden, prefix_len, valid_len))
    return (hidden_out, key_cache, value_cache)
```

```python
import jax
import jax.numpy as jnp
from jax import lax
from jax.sharding import PartitionSpec as P, NamedSharding

NORM_EPS = 1e-6
ROPE_BASE = 10000.0
MASK_FILL = -1e30


def rms_norm(acts, norm_scale):
    acts_f32 = acts.astype(jnp.float32)
    inv_rms = lax.rsqrt(jnp.mean(acts_f32 * acts_f32, axis=-1, keepdims=True) + NORM_EPS)
    return (acts_f32 * inv_rms * (1.0 + norm_scale.astype(jnp.float32))).astype(jnp.bfloat16)


def rope_tables(positions, head_dim):
    half_dim = head_dim // 2
    inv_freq = ROPE_BASE ** (-2.0 * jnp.arange(half_dim, dtype=jnp.float32) / head_dim)
    angles = positions.astype(jnp.float32)[:, None] * inv_freq[None, :]
    return jnp.cos(angles), jnp.sin(angles)


def apply_rope(vectors, cos_table, sin_table):
    half_dim = vectors.shape[-1] // 2
    first_half = vectors[..., :half_dim]
    second_half = vectors[..., half_dim:]
    return jnp.concatenate([first_half * cos_table - second_half * sin_table, second_half * cos_table + first_half * sin_table], axis=-1)


def dot(a, b):
    return jnp.dot(a, b, preferred_element_type=jnp.float32)


def solution(mesh):
    tp_size = mesh.shape["tp"]
    row_spec = P("dp", "tp", None)
    arg_specs = (row_spec, P("dp"), P("dp"), P(), P(None, "tp"), P(), P(), P("tp", None), P(), P(None, "tp"), P(None, "tp"), P("tp", None))
    chip_pairs = [(i, i ^ 2) for i in range(tp_size)]
    core_pairs = [(i, i ^ 1) for i in range(tp_size)]

    def swap_chip(a):
        return lax.ppermute(a, "tp", chip_pairs)

    def swap_core(a):
        return lax.ppermute(a, "tp", core_pairs)

    def local_layer(hidden, prefix_len, valid_len, norm_attn, w_query, w_key, w_value, w_out, norm_mlp, w_gate, w_up, w_down):
        num_batch, local_len, d_model = hidden.shape
        head_dim = w_key.shape[1]
        me = lax.axis_index("tp")
        my_pos = me * local_len + jnp.arange(local_len)
        cos_local, sin_local = rope_tables(my_pos, head_dim)

        w_query_x = swap_chip(w_query)
        w_out_x = swap_chip(w_out)
        w_query_c = swap_core(w_query)
        w_out_c = swap_core(w_out)

        normed = rms_norm(hidden, norm_attn).reshape(num_batch * local_len, d_model)
        key_local = apply_rope(dot(normed, w_key).reshape(num_batch, local_len, head_dim), cos_local, sin_local).astype(jnp.bfloat16)
        value_local = dot(normed, w_value).reshape(num_batch, local_len, head_dim).astype(jnp.bfloat16)
        key_x, value_x = swap_chip(key_local), swap_chip(value_local)
        key_c, value_c = swap_core(key_local), swap_core(value_local)
        w_query_xc = swap_core(w_query_x)
        w_out_xc = swap_core(w_out_x)
        key_xc, value_xc = swap_core(key_x), swap_core(value_x)
        w_gate_c, w_up_c, w_down_c = swap_core(w_gate), swap_core(w_up), swap_core(w_down)

        key_full = jnp.concatenate([key_local, key_c, key_x, key_xc], axis=1)
        value_full = jnp.concatenate([value_local, value_c, value_x, value_xc], axis=1)
        col_pos = jnp.concatenate([jnp.bitwise_xor(me, flip) * local_len + jnp.arange(local_len) for flip in (0, 1, 2, 3)])[None, None, :]
        row_pos = my_pos[None, :, None]
        allowed = (col_pos < valid_len[:, None, None]) & ((col_pos < prefix_len[:, None, None]) | (col_pos <= row_pos))

        attn_parts = []
        for w_q in (w_query, w_query_c, w_query_x, w_query_xc):
            heads = w_q.shape[1] // head_dim
            query = dot(normed, w_q).reshape(num_batch, local_len, heads, head_dim)
            query = (apply_rope(query, cos_local[:, None, :], sin_local[:, None, :]) * head_dim ** -0.5).astype(jnp.bfloat16)
            scores = jnp.einsum("bqhe,bke->bhqk", query, key_full, preferred_element_type=jnp.float32)
            probs = jax.nn.softmax(jnp.where(allowed[:, None], scores, MASK_FILL), axis=-1).astype(jnp.bfloat16)
            vals = jnp.einsum("bhqk,bke->bqhe", probs, value_full, preferred_element_type=jnp.float32).astype(jnp.bfloat16)
            attn_parts.append(vals.reshape(num_batch * local_len, heads * head_dim))
        attn_vals = jnp.concatenate(attn_parts, axis=1)
        w_out_full = jnp.concatenate([w_out, w_out_c, w_out_x, w_out_xc], axis=0)
        attn_out = dot(attn_vals, w_out_full).astype(jnp.bfloat16)
        hidden_mid = (hidden.reshape(-1, d_model).astype(jnp.float32) + attn_out.astype(jnp.float32)).astype(jnp.bfloat16)
        normed_mlp = rms_norm(hidden_mid, norm_mlp)

        half = normed_mlp.shape[0] // 2
        mine = [normed_mlp[:half], normed_mlp[half:]]
        mids = [hidden_mid[:half], hidden_mid[half:]]
        theirs = [swap_chip(m) for m in mine]

        def mlp(rows):
            total = None
            for w_g, w_u, w_d in ((w_gate, w_up, w_down), (w_gate_c, w_up_c, w_down_c)):
                act = (jax.nn.gelu(dot(rows, w_g), approximate=True) * dot(rows, w_u)).astype(jnp.bfloat16)
                part = dot(act, w_d)
                total = part if total is None else total + part
            return total

        own_a = mlp(mine[0])
        their_a = swap_chip(mlp(theirs[0]).astype(jnp.bfloat16))
        their_b_part = mlp(theirs[1]).astype(jnp.bfloat16)
        their_b = swap_chip(their_b_part)
        mine_b, _ = lax.optimization_barrier((mine[1], their_b_part))
        own_b = mlp(mine_b)
        outs = []
        for mid, own, their in ((mids[0], own_a, their_a), (mids[1], own_b, their_b)):
            mlp_out = (own + their.astype(jnp.float32)).astype(jnp.bfloat16)
            outs.append((mid.astype(jnp.float32) + mlp_out.astype(jnp.float32)).astype(jnp.bfloat16))
        hidden_out = jnp.concatenate(outs, axis=0).reshape(num_batch, local_len, d_model)
        return hidden_out, key_local, value_local

    return jax.shard_map(local_layer, mesh=mesh, in_specs=arg_specs, out_specs=(row_spec, row_spec, row_spec), check_vma=False)
```

```python
import functools

import jax
import jax.numpy as jnp
from jax import lax
from jax.experimental import pallas as pl
from jax.experimental.pallas import tpu as pltpu
from jax.sharding import PartitionSpec as P

NORM_EPS = 1e-6
ROPE_BASE = 10000.0
MASK_FILL = -1e30
GELU_A = 0.7978845608028654
GELU_B = 0.7978845608028654 * 0.044715
MIB = 1024 * 1024

F_TILE = 512
ROW_BLOCK = 448


ANY = pl.BlockSpec(memory_space=pl.ANY)
SMEM = pl.BlockSpec(memory_space=pltpu.SMEM)


def params(limit_mib, **kw):
    return pltpu.CompilerParams(vmem_limit_bytes=limit_mib * MIB, **kw)


def cost(flops, nbytes):
    return pl.CostEstimate(flops=int(flops), bytes_accessed=int(nbytes), transcendentals=0)


def fdot(a, b):
    return jnp.dot(a, b, preferred_element_type=jnp.float32)


def rope_tables(positions, head_dim):
    half_dim = head_dim // 2
    inv_freq = ROPE_BASE ** (-2.0 * jnp.arange(half_dim, dtype=jnp.float32) / head_dim)
    angles = positions.astype(jnp.float32)[:, None] * inv_freq[None, :]
    return jnp.cos(angles), jnp.sin(angles)


def norm_rows(acts, gain):
    inv_rms = lax.rsqrt(jnp.mean(acts * acts, axis=-1, keepdims=True) + NORM_EPS)
    return (acts * inv_rms * gain).astype(jnp.bfloat16)


def rope_halves(vec, cos, sin):
    half = vec.shape[-1] // 2
    a, c = vec[..., :half], vec[..., half:]
    return a * cos - c * sin, c * cos + a * sin


def kv_kernel(h_ref, gain_ref, wk_ref, wv_ref, cos_ref, sin_ref, x_ref, k_ref, v_ref):
    nb, rows, d = h_ref.shape
    gain = 1.0 + gain_ref[...].astype(jnp.float32)
    for b in range(nb):
        x_ref[b] = norm_rows(h_ref[b].astype(jnp.float32), gain)
    x = x_ref[...].reshape(nb * rows, d)
    key = fdot(x, wk_ref[...]).reshape(nb, rows, -1)
    lo, hi = rope_halves(key, cos_ref[...][None], sin_ref[...][None])
    half = lo.shape[-1]
    k_ref[:, :, :half] = lo.astype(jnp.bfloat16)
    k_ref[:, :, half:] = hi.astype(jnp.bfloat16)
    v_ref[...] = fdot(x, wv_ref[...]).astype(jnp.bfloat16).reshape(nb, rows, -1)


def kv_call(hidden, gain, w_key, w_value, cos, sin):
    nb, rows, d = hidden.shape
    hd = w_key.shape[1]
    step = ROW_BLOCK // rows
    full = lambda *shape: pl.BlockSpec(shape, lambda i: (0,) * len(shape))
    blk = lambda w: pl.BlockSpec((step, rows, w), lambda i: (i, 0, 0))
    return pl.pallas_call(
        kv_kernel,
        grid=(nb // step,),
        in_specs=[blk(d), full(1, d), full(d, hd), full(d, hd), full(rows, hd // 2), full(rows, hd // 2)],
        out_specs=[blk(d), blk(hd), blk(hd)],
        out_shape=[jax.ShapeDtypeStruct((nb, rows, w), jnp.bfloat16) for w in (d, hd, hd)],
        compiler_params=params(40),
        cost_estimate=cost(4 * nb * rows * d * hd, 4 * nb * rows * d),
        name="kv_proj",
    )(hidden, gain, w_key, w_value, cos, sin)


def query_kernel(head_dim, x_ref, w0_ref, w1_ref, cos_ref, sin_ref, q_ref):
    nb, rows, d = x_ref.shape
    x = x_ref[...].reshape(nb * rows, d)
    cos, sin = cos_ref[...][None], sin_ref[...][None]
    scale = head_dim ** -0.5
    half = head_dim // 2
    head = 0
    for w_ref in (w0_ref, w1_ref):
        for h in range(w_ref.shape[1] // head_dim):
            vec = fdot(x, w_ref[:, h * head_dim:(h + 1) * head_dim]).reshape(nb, rows, head_dim)
            lo, hi = rope_halves(vec, cos, sin)
            q_ref[:, head, :, :half] = (lo * scale).astype(jnp.bfloat16)
            q_ref[:, head, :, half:] = (hi * scale).astype(jnp.bfloat16)
            head += 1


def query_call(x, w0, w1, cos, sin, head_dim):
    nb, rows, d = x.shape
    width = w0.shape[1]
    heads = 2 * width // head_dim
    step = ROW_BLOCK // rows
    full = lambda *shape: pl.BlockSpec(shape, lambda i: (0,) * len(shape))
    return pl.pallas_call(
        functools.partial(query_kernel, head_dim),
        grid=(nb // step,),
        in_specs=[pl.BlockSpec((step, rows, d), lambda i: (i, 0, 0)), full(d, width), full(d, width),
                  full(rows, head_dim // 2), full(rows, head_dim // 2)],
        out_specs=pl.BlockSpec((step, heads, rows, head_dim), lambda i: (i, 0, 0, 0)),
        out_shape=jax.ShapeDtypeStruct((nb, heads, rows, head_dim), jnp.bfloat16),
        compiler_params=params(40),
        cost_estimate=cost(4 * nb * rows * d * width, 2 * nb * rows * d),
        name="query_proj",
    )(x, w0, w1, cos, sin)


def attn_kernel(base, pos_ref, pre_ref, val_ref, qa_ref, qb_ref, k0, k1, k2, k3, v0, v1, v2, v3, o_ref, k_scr, v_scr):
    _, heads, rows, hd = qa_ref.shape
    b = pl.program_id(0) + base
    for p, (k_ref, v_ref) in enumerate(((k0, v0), (k1, v1), (k2, v2), (k3, v3))):
        k_scr[p * rows:(p + 1) * rows] = k_ref[0]
        v_scr[p * rows:(p + 1) * rows] = v_ref[0]
    seq = 4 * rows
    col = lax.broadcasted_iota(jnp.int32, (rows, seq), 1)
    row = lax.broadcasted_iota(jnp.int32, (rows, seq), 0) + pos_ref[0]
    start = jnp.full((rows, seq), pos_ref[0], jnp.int32)
    for p in range(1, 4):
        start = jnp.where(col >= p * rows, pos_ref[p] - p * rows, start)
    col = col + start
    allowed = (col < val_ref[b]) & ((col < pre_ref[b]) | (col <= row))
    bias = jnp.where(allowed, 0.0, MASK_FILL).astype(jnp.float32)[None]
    keys, vals = k_scr[...], v_scr[...]
    head = 0
    for q_ref in (qa_ref, qb_ref):
        for g in range(0, heads, 2):
            q = q_ref[0, g:g + 2].reshape(2 * rows, hd)
            s = lax.dot_general(q, keys, (((1,), (1,)), ((), ())), preferred_element_type=jnp.float32)
            s = jnp.where(bias < 0.0, MASK_FILL, s.reshape(2, rows, seq))
            e = jnp.exp(s - jnp.max(s, axis=-1, keepdims=True))
            pr = (e * (1.0 / jnp.sum(e, axis=-1, keepdims=True))).astype(jnp.bfloat16)
            o = fdot(pr.reshape(2 * rows, seq), vals).astype(jnp.bfloat16)
            for i in range(2):
                o_ref[0, :, (head + i) * hd:(head + i + 1) * hd] = o[i * rows:(i + 1) * rows]
            head += 2


def attn_call(base, count, pos, prefix_len, valid_len, qa, qb, keys, vals):
    nb, heads, rows, hd = qa.shape
    d = 2 * heads * hd
    q_spec = pl.BlockSpec((1, heads, rows, hd), lambda i: (i + base, 0, 0, 0))
    kv_spec = pl.BlockSpec((1, rows, hd), lambda i: (i + base, 0, 0))
    return pl.pallas_call(
        functools.partial(attn_kernel, base),
        grid=(count,),
        in_specs=[SMEM] * 3 + [q_spec] * 2 + [kv_spec] * 8,
        out_specs=pl.BlockSpec((1, rows, d), lambda i: (i, 0, 0)),
        out_shape=jax.ShapeDtypeStruct((count, rows, d), jnp.bfloat16),
        scratch_shapes=[pltpu.VMEM((4 * rows, hd), jnp.bfloat16)] * 2,
        compiler_params=params(40),
        cost_estimate=cost(4 * count * 2 * heads * rows * 4 * rows * hd * 2, 8 * count * rows * d),
        name="attention",
    )(pos, prefix_len, valid_len, qa, qb, *keys, *vals)


def out_kernel(o_ref, h_ref, w0, w1, w2, w3, gain_ref, mid_ref, x_ref):
    nb, rows, d = o_ref.shape
    gain = 1.0 + gain_ref[...].astype(jnp.float32)
    pair = 2
    for b in range(0, nb, pair):
        o = o_ref[b:b + pair].reshape(pair * rows, d)
        total = None
        for p, w_ref in enumerate((w0, w1, w2, w3)):
            k = w_ref.shape[0]
            part = fdot(o[:, p * k:(p + 1) * k], w_ref[...])
            total = part if total is None else total + part
        res = h_ref[b:b + pair].reshape(pair * rows, d).astype(jnp.float32)
        mid = (res + total.astype(jnp.bfloat16).astype(jnp.float32)).astype(jnp.bfloat16)
        mid_ref[b * rows:(b + pair) * rows] = mid
        x_ref[b * rows:(b + pair) * rows] = norm_rows(mid.astype(jnp.float32), gain)


def out_call(base, o, hidden, w_parts, gain):
    count, rows, d = o.shape
    step = ROW_BLOCK // rows
    off = base // step
    full = lambda *shape: pl.BlockSpec(shape, lambda i: (0,) * len(shape))
    res_spec = pl.BlockSpec((ROW_BLOCK, d), lambda i: (i, 0))
    return pl.pallas_call(
        out_kernel,
        grid=(count // step,),
        in_specs=[pl.BlockSpec((step, rows, d), lambda i: (i, 0, 0)),
                  pl.BlockSpec((step, rows, d), lambda i: (i + off, 0, 0))]
        + [full(*w.shape) for w in w_parts] + [full(1, d)],
        out_specs=[res_spec, res_spec],
        out_shape=[jax.ShapeDtypeStruct((count * rows, d), jnp.bfloat16)] * 2,
        compiler_params=params(56),
        cost_estimate=cost(2 * count * rows * d * d, 8 * count * rows * d),
        name="out_proj",
    )(o, hidden, *w_parts, gain)


def mlp_kernel(mode, x_ref, wg0, wu0, wd0, wg1, wu1, wd1, *rest):
    if mode == "final":
        mid_hbm, their_hbm, _, out_hbm, gb, ub, db, acc, mid, their, sems, sem_in = rest
    else:
        _, out_ref, gb, ub, db, acc, sems = rest
        if mode == "f32":
            acc = out_ref
    m, d = x_ref.shape
    tiles = wg0.shape[1] // F_TILE
    steps = 2 * tiles

    def copies(wg, wu, wd, t, slot):
        cols = pl.ds(pl.multiple_of(t * F_TILE, F_TILE), F_TILE)
        return (
            pltpu.make_async_copy(wg.at[:, cols], gb.at[slot], sems.at[slot, 0]),
            pltpu.make_async_copy(wu.at[:, cols], ub.at[slot], sems.at[slot, 1]),
            pltpu.make_async_copy(wd.at[cols, :], db.at[slot], sems.at[slot, 2]),
        )

    def start(j, slot):
        @pl.when(j < tiles)
        def _():
            for c in copies(wg0, wu0, wd0, j, slot):
                c.start()

        @pl.when(j >= tiles)
        def _():
            for c in copies(wg1, wu1, wd1, j - tiles, slot):
                c.start()

    start(jnp.int32(0), 0)
    if mode == "final":
        ins = (pltpu.make_async_copy(mid_hbm, mid, sem_in.at[0]), pltpu.make_async_copy(their_hbm, their, sem_in.at[1]))
        for c in ins:
            c.start()
    acc[...] = jnp.zeros_like(acc)

    def body(j, carry):
        slot = lax.rem(j, 2)

        @pl.when(j + 1 < steps)
        def _():
            start(j + 1, 1 - slot)

        for c in copies(wg0, wu0, wd0, 0, slot):
            c.wait()
        acts = []
        for r in range(0, m, ROW_BLOCK):
            x = x_ref[r:r + ROW_BLOCK]
            g = fdot(x, gb[slot])
            u = fdot(x, ub[slot])
            t = jnp.tanh(g * (GELU_A + GELU_B * (g * g)))
            acts.append((g * (0.5 + 0.5 * t) * u).astype(jnp.bfloat16))
        for i, r in enumerate(range(0, m, ROW_BLOCK)):
            acc[r:r + ROW_BLOCK] += fdot(acts[i], db[slot])
        return carry

    lax.fori_loop(0, steps, body, 0)
    if mode == "bf16":
        out_ref[...] = acc[...].astype(jnp.bfloat16)
    if mode == "final":
        for c in ins:
            c.wait()
        mlp_out = (acc[...] + their[...].astype(jnp.float32)).astype(jnp.bfloat16)
        mid[...] = (mid[...].astype(jnp.float32) + mlp_out.astype(jnp.float32)).astype(jnp.bfloat16)
        done = pltpu.make_async_copy(mid, out_hbm.at[pl.ds(out_hbm.shape[0] - m, m)], sem_in.at[0])
        done.start()
        done.wait()


def mlp_call(mode, x, own, other, after, mid=None, their=None):
    m, d = x.shape
    f = own[0].shape[1]
    vmem = pl.BlockSpec(memory_space=pltpu.VMEM)
    scratch = [pltpu.VMEM((2, d, F_TILE), jnp.bfloat16)] * 2 + [pltpu.VMEM((2, F_TILE, d), jnp.bfloat16)]
    args = [x, *own, *other]
    specs = [vmem] + [ANY] * 6
    aliases = {}
    if mode == "final":
        args += [mid, their]
        specs += [ANY] * 2
        aliases = {len(args): 0}
        out_shape = jax.ShapeDtypeStruct(after.shape, jnp.bfloat16)
        out_spec = ANY
    else:
        out_shape = jax.ShapeDtypeStruct((m, d), jnp.float32 if mode == "f32" else jnp.bfloat16)
        out_spec = vmem
    args.append(after)
    specs.append(ANY)
    scratch.append(pltpu.VMEM((8, 128) if mode == "f32" else (m, d), jnp.float32))
    if mode == "final":
        scratch += [pltpu.VMEM((m, d), jnp.bfloat16)] * 2
    scratch.append(pltpu.SemaphoreType.DMA((2, 3)))
    if mode == "final":
        scratch.append(pltpu.SemaphoreType.DMA((2,)))
    return pl.pallas_call(
        functools.partial(mlp_kernel, mode),
        in_specs=specs,
        out_specs=out_spec,
        out_shape=out_shape,
        scratch_shapes=scratch,
        input_output_aliases=aliases,
        compiler_params=params(60),
        cost_estimate=cost(12 * m * d * f, 12 * d * f),
        name="mlp_" + mode,
    )(*args)


def combine_kernel(mid_ref, own_ref, their_ref, out_ref):
    mlp_out = (own_ref[...] + their_ref[...].astype(jnp.float32)).astype(jnp.bfloat16)
    out_ref[...] = (mid_ref[...].astype(jnp.float32) + mlp_out.astype(jnp.float32)).astype(jnp.bfloat16)


def combine_call(mid, own, their, total_rows, after):
    m, d = mid.shape
    blk = pl.BlockSpec((ROW_BLOCK // 2, d), lambda i: (i, 0))
    return pl.pallas_call(
        lambda a, b, c, _, o: combine_kernel(a, b, c, o),
        grid=(m // (ROW_BLOCK // 2),),
        in_specs=[blk] * 3 + [ANY],
        out_specs=blk,
        out_shape=jax.ShapeDtypeStruct((total_rows, d), jnp.bfloat16),
        compiler_params=params(40),
        cost_estimate=cost(4 * m * d, 10 * m * d),
        name="combine",
    )(mid, own, their, after)


def solution(mesh):
    tp_size = mesh.shape["tp"]
    row_spec = P("dp", "tp", None)
    arg_specs = (row_spec, P("dp"), P("dp"), P(), P(None, "tp"), P(), P(), P("tp", None), P(), P(None, "tp"), P(None, "tp"), P("tp", None))
    chip_pairs = [(i, i ^ 2) for i in range(tp_size)]
    core_pairs = [(i, i ^ 1) for i in range(tp_size)]

    def swap_chip(a):
        return lax.ppermute(a, "tp", chip_pairs)

    def swap_core(a):
        return lax.ppermute(a, "tp", core_pairs)

    def local_layer(hidden, prefix_len, valid_len, norm_attn, w_query, w_key, w_value, w_out, norm_mlp, w_gate, w_up, w_down):
        nb, rows, d = hidden.shape
        head_dim = w_key.shape[1]
        half = nb // 2
        me = lax.axis_index("tp")
        cos, sin = rope_tables(me * rows + jnp.arange(rows), head_dim)
        pos = jnp.bitwise_xor(me, jnp.arange(tp_size, dtype=jnp.int32)) * rows

        w_query_x = swap_chip(w_query)
        w_query_c = swap_core(w_query)
        w_out_c = swap_core(w_out)
        normed, key_local, value_local = kv_call(hidden, norm_attn[None], w_key, w_value, cos, sin)
        key_x, value_x = swap_chip(key_local), swap_chip(value_local)
        key_c, value_c = swap_core(key_local), swap_core(value_local)
        w_out_late, _ = lax.optimization_barrier((w_out, key_local))
        w_out_x = swap_chip(w_out_late)
        w_query_xc = swap_core(w_query_x)
        query_a = query_call(normed, w_query, w_query_c, cos, sin, head_dim)
        w_gate_c, w_up_c, w_down_c = swap_core(w_gate), swap_core(w_up), swap_core(w_down)
        query_b = query_call(normed, w_query_x, w_query_xc, cos, sin, head_dim)
        key_xc, value_xc = swap_core(key_x), swap_core(value_x)
        w_out_xc = swap_core(w_out_x)

        keys = (key_local, key_c, key_x, key_xc)
        vals = (value_local, value_c, value_x, value_xc)
        w_outs = (w_out, w_out_c, w_out_x, w_out_xc)
        mids, mine = [], []
        for base in (0, half):
            o = attn_call(base, half, pos, prefix_len, valid_len, query_a, query_b, keys, vals)
            mid, x = out_call(base, o, hidden, w_outs, norm_mlp[None])
            mids.append(mid)
            mine.append(x)
        theirs = [swap_chip(x) for x in mine]

        own = (w_gate, w_up, w_down)
        other = (w_gate_c, w_up_c, w_down_c)
        own_a = mlp_call("f32", mine[0], own, other, mine[1])
        part_a = mlp_call("bf16", theirs[0], own, other, own_a)
        their_a = swap_chip(part_a)
        part_b = mlp_call("bf16", theirs[1], own, other, part_a)
        their_b = swap_chip(part_b)
        out = combine_call(mids[0], own_a, their_a, nb * rows, part_b)
        out = mlp_call("final", mine[1], own, other, out, mids[1], their_b)
        return out.reshape(nb, rows, d), key_local, value_local

    return jax.shard_map(local_layer, mesh=mesh, in_specs=arg_specs, out_specs=(row_spec, row_spec, row_spec), check_vma=False)
```

```python
import functools

import jax
import jax.numpy as jnp
from jax import lax
from jax.experimental import pallas as pl
from jax.experimental.pallas import tpu as pltpu
from jax.sharding import PartitionSpec as P


NORM_EPS = 1e-6
ROPE_BASE = 10000.0
MASK_FILL = -1e30
GELU_A = 0.7978845608028654
GELU_B = 0.7978845608028654 * 0.044715
MIB = 1024 * 1024

F_TILE = 512
ROW_BLOCK = 448

VMEM_MIB = 63


ANY = pl.BlockSpec(memory_space=pl.ANY)
SMEM = pl.BlockSpec(memory_space=pltpu.SMEM)


def params(limit_mib, **kw):
    return pltpu.CompilerParams(vmem_limit_bytes=limit_mib * MIB, **kw)


def cost(flops, nbytes):
    return pl.CostEstimate(flops=int(flops), bytes_accessed=int(nbytes), transcendentals=0)


def fdot(a, b):
    return jnp.dot(a, b, preferred_element_type=jnp.float32)


def rope_tables(positions, head_dim):
    half_dim = head_dim // 2
    inv_freq = ROPE_BASE ** (-2.0 * jnp.arange(half_dim, dtype=jnp.float32) / head_dim)
    angles = positions.astype(jnp.float32)[:, None] * inv_freq[None, :]
    return jnp.cos(angles), jnp.sin(angles)


def norm_rows(acts, gain):
    inv_rms = lax.rsqrt(jnp.mean(acts * acts, axis=-1, keepdims=True) + NORM_EPS)
    return (acts * inv_rms * gain).astype(jnp.bfloat16)


def rope_halves(vec, cos, sin):
    half = vec.shape[-1] // 2
    a, c = vec[..., :half], vec[..., half:]
    return a * cos - c * sin, c * cos + a * sin


def kv_kernel(h_ref, gain_ref, wk_ref, wv_ref, cos_ref, sin_ref, x_ref, k_ref, v_ref, kva_ref, kvb_ref):
    nb, rows, d = h_ref.shape
    gain = 1.0 + gain_ref[...].astype(jnp.float32)
    for b in range(nb):
        x_ref[b] = norm_rows(h_ref[b].astype(jnp.float32), gain)
    x = x_ref[...].reshape(nb * rows, d)
    key = fdot(x, wk_ref[...]).reshape(nb, rows, -1)
    lo, hi = rope_halves(key, cos_ref[...][None], sin_ref[...][None])
    half = lo.shape[-1]
    k_ref[:, :, :half] = lo.astype(jnp.bfloat16)
    k_ref[:, :, half:] = hi.astype(jnp.bfloat16)
    v_ref[...] = fdot(x, wv_ref[...]).astype(jnp.bfloat16).reshape(nb, rows, -1)
    first = pl.program_id(0) < pl.num_programs(0) // 2

    @pl.when(first)
    def _():
        kva_ref[:, :, :2 * half] = k_ref[...]
        kva_ref[:, :, 2 * half:] = v_ref[...]

    @pl.when(jnp.logical_not(first))
    def _():
        kvb_ref[:, :, :2 * half] = k_ref[...]
        kvb_ref[:, :, 2 * half:] = v_ref[...]


def kv_call(hidden, gain, w_key, w_value, cos, sin):
    nb, rows, d = hidden.shape
    hd = w_key.shape[1]
    step = ROW_BLOCK // rows
    steps = nb // step
    full = lambda *shape: pl.BlockSpec(shape, lambda i: (0,) * len(shape))
    blk = lambda w: pl.BlockSpec((step, rows, w), lambda i: (i, 0, 0))
    kva = pl.BlockSpec((step, rows, 2 * hd), lambda i: (jnp.minimum(i, steps // 2 - 1), 0, 0))
    kvb = pl.BlockSpec((step, rows, 2 * hd), lambda i: (jnp.maximum(i - steps // 2, 0), 0, 0))
    return pl.pallas_call(
        kv_kernel,
        grid=(steps,),
        in_specs=[blk(d), full(1, d), full(d, hd), full(d, hd), full(rows, hd // 2), full(rows, hd // 2)],
        out_specs=[blk(d), blk(hd), blk(hd), kva, kvb],
        out_shape=[jax.ShapeDtypeStruct((n, rows, w), jnp.bfloat16) for n, w in ((nb, d), (nb, hd), (nb, hd), (nb // 2, 2 * hd), (nb // 2, 2 * hd))],
        compiler_params=params(VMEM_MIB),
        cost_estimate=cost(4 * nb * rows * d * hd, 4 * nb * rows * d),
        name="kv_proj",
    )(hidden, gain, w_key, w_value, cos, sin)


def load_parts(parts, dst, sems, offsets):
    for i, (ref, off) in enumerate(zip(parts, offsets)):
        pltpu.make_async_copy(ref, dst.at[pl.ds(off, ref.shape[0])], sems.at[i]).start()
    for i, (ref, off) in enumerate(zip(parts, offsets)):
        pltpu.make_async_copy(ref, dst.at[pl.ds(off, ref.shape[0])], sems.at[i]).wait()


def query_body(head_dim, x_ref, weights, cos_ref, sin_ref, q_ref):
    nb, rows, d = x_ref.shape
    x = x_ref[...].reshape(nb * rows, d)
    cos, sin = cos_ref[...][None], sin_ref[...][None]
    scale = head_dim ** -0.5
    half = head_dim // 2
    for head in range(q_ref.shape[1]):
        vec = fdot(x, weights(head)).reshape(nb, rows, head_dim)
        lo, hi = rope_halves(vec, cos, sin)
        q_ref[:, head, :, :half] = (lo * scale).astype(jnp.bfloat16)
        q_ref[:, head, :, half:] = (hi * scale).astype(jnp.bfloat16)


def query_near_kernel(head_dim, x_ref, w0_ref, w1_ref, cos_ref, sin_ref, q_ref):
    per = w0_ref.shape[1] // head_dim

    def weights(head):
        ref = (w0_ref, w1_ref)[head // per]
        return ref[:, (head % per) * head_dim:(head % per + 1) * head_dim]

    query_body(head_dim, x_ref, weights, cos_ref, sin_ref, q_ref)


def query_far_kernel(head_dim, group_ref, x_ref, *rest):
    pieces, (cos_ref, sin_ref, q_ref, w_scr, sems) = rest[:8], rest[8:]
    size = pieces[0].shape[0]
    span = 4 * size

    @pl.when(pl.program_id(0) == 0)
    def _():
        offs = [pl.multiple_of(group_ref[k] * size, size) + s * span for s in range(2) for k in range(4)]
        load_parts(pieces, w_scr, sems, offs)

    per = w_scr.shape[1] // head_dim

    def weights(head):
        s = head // per
        return w_scr[s * span:(s + 1) * span, (head % per) * head_dim:(head % per + 1) * head_dim]

    query_body(head_dim, x_ref, weights, cos_ref, sin_ref, q_ref)


def query_call(x, weights, cos, sin, head_dim, group=None):
    nb, rows, d = x.shape
    width = weights[0].shape[1]
    heads = 2 * width // head_dim
    step = ROW_BLOCK // rows
    full = lambda *shape: pl.BlockSpec(shape, lambda i: (0,) * len(shape))
    x_spec = pl.BlockSpec((step, rows, d), lambda i: (i, 0, 0))
    tabs = [full(rows, head_dim // 2)] * 2
    if group is None:
        kernel, specs, args, scratch = query_near_kernel, [x_spec] + [full(d, width)] * 2 + tabs, (x, *weights, cos, sin), []
    else:
        kernel, specs, args = query_far_kernel, [SMEM, x_spec] + [ANY] * 8 + tabs, (group, x, *weights, cos, sin)
        scratch = [pltpu.VMEM((2 * d, width), jnp.bfloat16), pltpu.SemaphoreType.DMA((8,))]
    return pl.pallas_call(
        functools.partial(kernel, head_dim),
        grid=(nb // step,),
        in_specs=specs,
        out_specs=pl.BlockSpec((step, heads, rows, head_dim), lambda i: (i, 0, 0, 0)),
        out_shape=jax.ShapeDtypeStruct((nb, heads, rows, head_dim), jnp.bfloat16),
        scratch_shapes=scratch,
        compiler_params=params(VMEM_MIB),
        cost_estimate=cost(4 * nb * rows * d * width, 2 * nb * rows * d),
        name="query_near" if group is None else "query_far",
    )(*args)


def attn_kernel(base, pos_ref, pre_ref, val_ref, qa_ref, qb_ref, kv0, kv1, kv2, kv3, o_ref, k_scr, v_scr):
    _, heads, rows, hd = qa_ref.shape
    b = pl.program_id(0) + base
    for p, kv_ref in enumerate((kv0, kv1, kv2, kv3)):
        k_scr[p * rows:(p + 1) * rows] = kv_ref[0, :, :hd]
        v_scr[p * rows:(p + 1) * rows] = kv_ref[0, :, hd:]
    seq = 4 * rows
    col = lax.broadcasted_iota(jnp.int32, (rows, seq), 1)
    row = lax.broadcasted_iota(jnp.int32, (rows, seq), 0) + pos_ref[0]
    start = jnp.full((rows, seq), pos_ref[0], jnp.int32)
    for p in range(1, 4):
        start = jnp.where(col >= p * rows, pos_ref[p] - p * rows, start)
    col = col + start
    allowed = (col < val_ref[b]) & ((col < pre_ref[b]) | (col <= row))
    bias = jnp.where(allowed, 0.0, MASK_FILL).astype(jnp.float32)[None]
    keys, vals = k_scr[...], v_scr[...]
    head = 0
    for q_ref in (qa_ref, qb_ref):
        for g in range(0, heads, 2):
            q = q_ref[0, g:g + 2].reshape(2 * rows, hd)
            s = lax.dot_general(q, keys, (((1,), (1,)), ((), ())), preferred_element_type=jnp.float32)
            s = jnp.where(bias < 0.0, MASK_FILL, s.reshape(2, rows, seq))
            e = jnp.exp(s - jnp.max(s, axis=-1, keepdims=True))
            pr = (e * (1.0 / jnp.sum(e, axis=-1, keepdims=True))).astype(jnp.bfloat16)
            o = fdot(pr.reshape(2 * rows, seq), vals).astype(jnp.bfloat16)
            for i in range(2):
                o_ref[0, :, (head + i) * hd:(head + i + 1) * hd] = o[i * rows:(i + 1) * rows]
            head += 2


def attn_call(base, count, pos, prefix_len, valid_len, qa, qb, kvs):
    _, heads, rows, hd = qa.shape
    d = 2 * heads * hd
    q_spec = pl.BlockSpec((1, heads, rows, hd), lambda i: (i + base, 0, 0, 0))
    kv_spec = pl.BlockSpec((1, rows, 2 * hd), lambda i: (i, 0, 0))
    return pl.pallas_call(
        functools.partial(attn_kernel, base),
        grid=(count,),
        in_specs=[SMEM] * 3 + [q_spec] * 2 + [kv_spec] * 4,
        out_specs=pl.BlockSpec((1, rows, d), lambda i: (i, 0, 0)),
        out_shape=jax.ShapeDtypeStruct((count, rows, d), jnp.bfloat16),
        scratch_shapes=[pltpu.VMEM((4 * rows, hd), jnp.bfloat16)] * 2,
        compiler_params=params(VMEM_MIB),
        cost_estimate=cost(4 * count * 2 * heads * rows * 4 * rows * hd * 2, 8 * count * rows * d),
        name="attention",
    )(pos, prefix_len, valid_len, qa, qb, *kvs)


def out_kernel(group_ref, o_ref, h_ref, *rest):
    weights, gain_ref, mid_ref, x_ref, w_scr, sems = rest[:10], *rest[10:]
    nb, rows, d = o_ref.shape
    wide, size = weights[0].shape[0], weights[2].shape[0]

    @pl.when(pl.program_id(0) == 0)
    def _():
        offs = [0, wide] + [pl.multiple_of(group_ref[k] * size, size) + s * wide for s in (2, 3) for k in range(4)]
        load_parts(weights, w_scr, sems, offs)

    gain = 1.0 + gain_ref[...].astype(jnp.float32)
    pair = 2
    for b in range(0, nb, pair):
        total = fdot(o_ref[b:b + pair].reshape(pair * rows, d), w_scr[...])
        res = h_ref[b:b + pair].reshape(pair * rows, d).astype(jnp.float32)
        mid = (res + total.astype(jnp.bfloat16).astype(jnp.float32)).astype(jnp.bfloat16)
        mid_ref[b * rows:(b + pair) * rows] = mid
        x_ref[b * rows:(b + pair) * rows] = norm_rows(mid.astype(jnp.float32), gain)


def out_call(base, o, hidden, group, weights, gain):
    count, rows, d = o.shape
    step = ROW_BLOCK // rows
    off = base // step
    full = lambda *shape: pl.BlockSpec(shape, lambda i: (0,) * len(shape))
    res_spec = pl.BlockSpec((ROW_BLOCK, d), lambda i: (i, 0))
    return pl.pallas_call(
        out_kernel,
        grid=(count // step,),
        in_specs=[SMEM, pl.BlockSpec((step, rows, d), lambda i: (i, 0, 0)),
                  pl.BlockSpec((step, rows, d), lambda i: (i + off, 0, 0))]
        + [ANY] * 10 + [full(1, d)],
        out_specs=[res_spec, res_spec],
        out_shape=[jax.ShapeDtypeStruct((count * rows, d), jnp.bfloat16)] * 2,
        scratch_shapes=[pltpu.VMEM((d, d), jnp.bfloat16), pltpu.SemaphoreType.DMA((10,))],
        compiler_params=params(VMEM_MIB),
        cost_estimate=cost(2 * count * rows * d * d, 8 * count * rows * d),
        name="out_proj",
    )(group, o, hidden, *weights, gain)


def mlp_kernel(mode, num_x, num_sets, *refs):
    xs, refs = refs[:num_x], refs[num_x:]
    sets, refs = [refs[3 * i:3 * i + 3] for i in range(num_sets)], refs[3 * num_sets:]
    if mode in ("sum", "final"):
        part_hbm, refs = refs[0], refs[1:]
    if mode == "final":
        (mid_hbm, their_hbm), refs = refs[:2], refs[2:]
    _, out_hbm, x_ref, gb, ub, db, acc, stage, sems, sem_x, sem_in = refs[:11]
    bufs = refs[11:]
    m, _ = x_ref.shape
    tiles = sets[0][0].shape[1] // F_TILE
    steps = num_sets * tiles

    def copies(ws, t, slot):
        wg, wu, wd = ws
        cols = pl.ds(pl.multiple_of(t * F_TILE, F_TILE), F_TILE)
        return (
            pltpu.make_async_copy(wg.at[:, cols], gb.at[slot], sems.at[slot, 0]),
            pltpu.make_async_copy(wu.at[:, cols], ub.at[slot], sems.at[slot, 1]),
            pltpu.make_async_copy(wd.at[cols, :], db.at[slot], sems.at[slot, 2]),
        )

    def start(j, slot):
        for i in range(num_sets):
            @pl.when((j >= i * tiles) & (j < (i + 1) * tiles))
            def _():
                for c in copies(sets[i], j - i * tiles, slot):
                    c.start()

    offs, at = [], 0
    for ref in xs:
        offs.append(at)
        at += ref.shape[0]
    x_in = [pltpu.make_async_copy(ref, x_ref.at[pl.ds(off, ref.shape[0])], sem_x.at[i]) for i, (ref, off) in enumerate(zip(xs, offs))]
    for c in x_in:
        c.start()
    start(jnp.int32(0), 0)
    extra = []
    if mode in ("sum", "final"):
        row0 = part_hbm.shape[0] - m if mode == "sum" else 0
        extra.append(pltpu.make_async_copy(part_hbm.at[pl.ds(row0, m)], bufs[0], sem_in.at[0]))
    if mode == "final":
        extra.append(pltpu.make_async_copy(mid_hbm, stage, sem_in.at[1]))
        extra.append(pltpu.make_async_copy(their_hbm, bufs[1], sem_in.at[2]))
    acc[...] = jnp.zeros_like(acc)
    for c in x_in:
        c.wait()
    for c in extra:
        c.start()
    group = 2 * ROW_BLOCK

    def body(j, carry):
        slot = lax.rem(j, 2)

        @pl.when(j + 1 < steps)
        def _():
            start(j + 1, 1 - slot)

        for c in copies(sets[0], 0, slot):
            c.wait()

        def rows(r0):
            acts = []
            for r in range(0, group, ROW_BLOCK):
                x = x_ref[pl.ds(r0 + r, ROW_BLOCK)]
                g = fdot(x, gb[slot])
                u = fdot(x, ub[slot])
                t = jnp.tanh(g * (GELU_A + GELU_B * (g * g)))
                acts.append((g * (0.5 + 0.5 * t) * u).astype(jnp.bfloat16))
            for i, r in enumerate(range(0, group, ROW_BLOCK)):
                acc[pl.ds(r0 + r, ROW_BLOCK)] += fdot(acts[i], db[slot])

        if m == group:
            rows(0)
        else:
            @pl.loop(0, m // group)
            def _(i):
                rows(pl.multiple_of(i * group, group))
        return carry

    lax.fori_loop(0, steps, body, 0)
    for c in extra:
        c.wait()
    chunk = ROW_BLOCK // 2
    done = []
    for i, r in enumerate(range(0, m, chunk)):
        sl = pl.ds(r, chunk)
        total = acc[sl]
        if mode in ("sum", "final"):
            total = total + bufs[0][sl].astype(jnp.float32)
        if mode == "final":
            total = (total + bufs[1][sl].astype(jnp.float32)).astype(jnp.bfloat16).astype(jnp.float32)
            total = stage[sl].astype(jnp.float32) + total
        stage[sl] = total.astype(jnp.bfloat16)
        c = pltpu.make_async_copy(stage.at[sl], out_hbm.at[pl.ds(r, chunk)], sem_x.at[i])
        c.start()
        done.append(c)
    for c in done:
        c.wait()


def mlp_call(mode, xs, sets, after, part=None, mid=None, their=None, out_rows=None):
    m, d = sum(x.shape[0] for x in xs), xs[0].shape[1]
    f = sets[0][0].shape[1]
    args = [*xs] + [w for ws in sets for w in ws]
    if mode in ("sum", "final"):
        args.append(part)
    if mode == "final":
        args += [mid, their]
    args.append(after)
    scratch = [pltpu.VMEM((m, d), jnp.bfloat16)]
    scratch += [pltpu.VMEM((2, d, F_TILE), jnp.bfloat16)] * 2 + [pltpu.VMEM((2, F_TILE, d), jnp.bfloat16)]
    scratch += [pltpu.VMEM((m, d), jnp.float32), pltpu.VMEM((m, d), jnp.bfloat16)]
    scratch += [pltpu.SemaphoreType.DMA((2, 3)), pltpu.SemaphoreType.DMA((16,)), pltpu.SemaphoreType.DMA((3,))]
    scratch += [pltpu.VMEM((m, d), jnp.bfloat16)] * {"part": 0, "sum": 1, "final": 2}[mode]
    return pl.pallas_call(
        functools.partial(mlp_kernel, mode, len(xs), len(sets)),
        in_specs=[ANY] * len(args),
        out_specs=ANY,
        out_shape=jax.ShapeDtypeStruct((out_rows or m, d), jnp.bfloat16),
        scratch_shapes=scratch,
        compiler_params=params(VMEM_MIB),
        cost_estimate=cost(6 * len(sets) * m * d * f, 6 * len(sets) * d * f),
    )(*args)


def combine_kernel(mid_ref, own_ref, their_ref, _, out_ref):
    mlp_out = (own_ref[...].astype(jnp.float32) + their_ref[...].astype(jnp.float32)).astype(jnp.bfloat16)
    out_ref[...] = (mid_ref[...].astype(jnp.float32) + mlp_out.astype(jnp.float32)).astype(jnp.bfloat16)


def combine_call(mid, own, their, out):
    m, d = mid.shape
    step = ROW_BLOCK // 2
    off = (out.shape[0] - m) // step
    blk = pl.BlockSpec((step, d), lambda i: (i, 0))
    return pl.pallas_call(
        combine_kernel,
        grid=(m // step,),
        in_specs=[blk] * 3 + [ANY],
        out_specs=pl.BlockSpec((step, d), lambda i: (i + off, 0)),
        out_shape=jax.ShapeDtypeStruct(out.shape, jnp.bfloat16),
        input_output_aliases={3: 0},
        compiler_params=params(VMEM_MIB),
        cost_estimate=cost(4 * m * d, 8 * m * d),
        name="combine",
    )(mid, own, their, out)


def solution(mesh):
    tp_size, dp_size = mesh.shape["tp"], mesh.shape["dp"]
    row_spec = P("dp", "tp", None)
    arg_specs = (row_spec, P("dp"), P("dp"), P(), P(None, "tp"), P(), P(), P("tp", None), P(), P(None, "tp"), P(None, "tp"), P("tp", None))

    def swap(a, axis, bit):
        return lax.ppermute(a, axis, [(i, i ^ bit) for i in range(mesh.shape[axis])])

    def spread(w, me_dp):
        size = w.shape[0] // dp_size
        quarter = lax.dynamic_slice_in_dim(w, me_dp * size, size, axis=0)
        return swap(quarter, "tp", 2)

    def gather(got, diag_first):
        y = swap(got, "dp", 1)
        z = swap(got, "dp", 2)
        diag = swap(y, "dp", 2) if diag_first else swap(z, "dp", 1)
        far = [got, y, z, diag]
        return far + [swap(a, "tp", 1) for a in far]

    def local_layer(hidden, prefix_len, valid_len, norm_attn, w_query, w_key, w_value, w_out, norm_mlp, w_gate, w_up, w_down):
        nb, rows, d = hidden.shape
        head_dim = w_key.shape[1]
        half = nb // 2
        me, me_dp = lax.axis_index("tp"), lax.axis_index("dp")
        group = jnp.bitwise_xor(me_dp, jnp.arange(dp_size, dtype=jnp.int32))
        pos = jnp.bitwise_xor(me, jnp.arange(tp_size, dtype=jnp.int32)) * rows
        cos, sin = rope_tables(me * rows + jnp.arange(rows), head_dim)

        wq_got = spread(w_query, me_dp)
        wo_got = spread(w_out, me_dp)
        w_query_c = swap(w_query, "tp", 1)
        normed, key_local, value_local, kv_a, kv_b = kv_call(hidden, norm_attn[None], w_key, w_value, cos, sin)
        kvs = []
        for kv in (kv_a, kv_b):
            kv_x = swap(kv, "tp", 2)
            kvs.append((kv, swap(kv, "tp", 1), kv_x, swap(kv_x, "tp", 1)))
        query_a = query_call(normed, (w_query, w_query_c), cos, sin, head_dim)
        query_b = query_call(normed, gather(wq_got, True), cos, sin, head_dim, group)
        w_outs = [w_out, swap(w_out, "tp", 1)] + gather(wo_got, False)
        near = (w_gate, w_up, w_down)
        far = tuple(swap(w, "tp", 1) for w in near)

        mids, mine = [], []
        for base, kv in ((0, kvs[0]), (half, kvs[1])):
            o = attn_call(base, half, pos, prefix_len, valid_len, query_a, query_b, kv)
            mid, x = out_call(base, o, hidden, group, w_outs, norm_mlp[None])
            mids.append(mid)
            mine.append(x)
        theirs = [swap(x, "tp", 2) for x in mine]

        own = mlp_call("part", mine, [near], mine[1])
        part_a = mlp_call("part", theirs[:1], [near, far], own)
        their_a = swap(part_a, "tp", 2)
        part_b = mlp_call("part", theirs[1:], [near, far], part_a)
        their_b = swap(part_b, "tp", 2)
        out = mlp_call("final", mine[:1], [far], part_b, own, mids[0], their_a, nb * rows)
        own_b = mlp_call("sum", mine[1:], [far], out, own)
        out = combine_call(mids[1], own_b, their_b, out)
        return out.reshape(nb, rows, d), key_local, value_local

    return jax.shard_map(local_layer, mesh=mesh, in_specs=arg_specs, out_specs=(row_spec, row_spec, row_spec), check_vma=False)
```

```python
import functools

import jax
import jax.numpy as jnp
from jax import lax
from jax.experimental import pallas as pl
from jax.experimental.pallas import tpu as pltpu
from jax.sharding import PartitionSpec as P


NORM_EPS = 1e-6
ROPE_BASE = 10000.0
MASK_FILL = -1e30
GELU_A = 0.7978845608028654
GELU_B = 0.7978845608028654 * 0.044715

F_TILE = 512
ROW_BLOCK = 448

VMEM_LIMIT = 67043328
NUM_FAR = 10
NUM_WO = 2 + NUM_FAR
SPLIT_WAIT = False


ANY = pl.BlockSpec(memory_space=pl.ANY)
SMEM = pl.BlockSpec(memory_space=pltpu.SMEM)


def params(limit, **kw):
    return pltpu.CompilerParams(vmem_limit_bytes=limit, **kw)


def cost(flops, nbytes):
    return pl.CostEstimate(flops=int(flops), bytes_accessed=int(nbytes), transcendentals=0)


def fdot(a, b):
    return jnp.dot(a, b, preferred_element_type=jnp.float32)


def rope_tables(positions, head_dim):
    half_dim = head_dim // 2
    inv_freq = ROPE_BASE ** (-2.0 * jnp.arange(half_dim, dtype=jnp.float32) / head_dim)
    angles = positions.astype(jnp.float32)[:, None] * inv_freq[None, :]
    return jnp.cos(angles), jnp.sin(angles)


def norm_rows(acts, gain):
    inv_rms = lax.rsqrt(jnp.mean(acts * acts, axis=-1, keepdims=True) + NORM_EPS)
    return (acts * inv_rms * gain).astype(jnp.bfloat16)


def rope_halves(vec, cos, sin):
    half = vec.shape[-1] // 2
    a, c = vec[..., :half], vec[..., half:]
    return a * cos - c * sin, c * cos + a * sin


def kv_kernel(h_ref, gain_ref, wk_ref, wv_ref, cos_ref, sin_ref, x_ref, k_ref, v_ref, kva_ref, kvb_ref):
    nb, rows, d = h_ref.shape
    gain = 1.0 + gain_ref[...].astype(jnp.float32)
    for b in range(nb):
        x_ref[b] = norm_rows(h_ref[b].astype(jnp.float32), gain)
    x = x_ref[...].reshape(nb * rows, d)
    key = fdot(x, wk_ref[...]).reshape(nb, rows, -1)
    lo, hi = rope_halves(key, cos_ref[...][None], sin_ref[...][None])
    half = lo.shape[-1]
    k_ref[:, :, :half] = lo.astype(jnp.bfloat16)
    k_ref[:, :, half:] = hi.astype(jnp.bfloat16)
    v_ref[...] = fdot(x, wv_ref[...]).astype(jnp.bfloat16).reshape(nb, rows, -1)
    first = pl.program_id(0) < pl.num_programs(0) // 2

    @pl.when(first)
    def _():
        kva_ref[:, :, :2 * half] = k_ref[...]
        kva_ref[:, :, 2 * half:] = v_ref[...]

    @pl.when(jnp.logical_not(first))
    def _():
        kvb_ref[:, :, :2 * half] = k_ref[...]
        kvb_ref[:, :, 2 * half:] = v_ref[...]


def kv_call(hidden, gain, w_key, w_value, cos, sin):
    nb, rows, d = hidden.shape
    hd = w_key.shape[1]
    step = ROW_BLOCK // rows
    steps = nb // step
    full = lambda *shape: pl.BlockSpec(shape, lambda i: (0,) * len(shape))
    blk = lambda w: pl.BlockSpec((step, rows, w), lambda i: (i, 0, 0))
    kva = pl.BlockSpec((step, rows, 2 * hd), lambda i: (jnp.minimum(i, steps // 2 - 1), 0, 0))
    kvb = pl.BlockSpec((step, rows, 2 * hd), lambda i: (jnp.maximum(i - steps // 2, 0), 0, 0))
    return pl.pallas_call(
        kv_kernel,
        grid=(steps,),
        in_specs=[blk(d), full(1, d), full(d, hd), full(d, hd), full(rows, hd // 2), full(rows, hd // 2)],
        out_specs=[blk(d), blk(hd), blk(hd), kva, kvb],
        out_shape=[jax.ShapeDtypeStruct((n, rows, w), jnp.bfloat16) for n, w in ((nb, d), (nb, hd), (nb, hd), (nb // 2, 2 * hd), (nb // 2, 2 * hd))],
        compiler_params=params(VMEM_LIMIT),
        cost_estimate=cost(4 * nb * rows * d * hd, 4 * nb * rows * d),
        name="kv_proj",
    )(hidden, gain, w_key, w_value, cos, sin)


def load_parts(parts, dst, sems, offsets):
    for i, (ref, off) in enumerate(zip(parts, offsets)):
        pltpu.make_async_copy(ref, dst.at[pl.ds(off, ref.shape[0])], sems.at[i]).start()
    for i, (ref, off) in enumerate(zip(parts, offsets)):
        pltpu.make_async_copy(ref, dst.at[pl.ds(off, ref.shape[0])], sems.at[i]).wait()


def far_offsets(group_ref, span):
    size = span // 4
    offs = [pl.multiple_of(group_ref[k] * size, size) for k in range(4)]
    offs.append(pl.multiple_of(group_ref[3] * size + size // 2, size // 2))
    return offs + [o + span for o in offs]


def query_body(head_dim, x_ref, weights, cos_ref, sin_ref, q_ref):
    nb, rows, d = x_ref.shape
    x = x_ref[...].reshape(nb * rows, d)
    cos, sin = cos_ref[...][None], sin_ref[...][None]
    scale = head_dim ** -0.5
    half = head_dim // 2
    for head in range(q_ref.shape[1]):
        vec = fdot(x, weights(head)).reshape(nb, rows, head_dim)
        lo, hi = rope_halves(vec, cos, sin)
        q_ref[:, head, :, :half] = (lo * scale).astype(jnp.bfloat16)
        q_ref[:, head, :, half:] = (hi * scale).astype(jnp.bfloat16)


def query_near_kernel(head_dim, x_ref, w0_ref, w1_ref, cos_ref, sin_ref, q_ref):
    per = w0_ref.shape[1] // head_dim

    def weights(head):
        ref = (w0_ref, w1_ref)[head // per]
        return ref[:, (head % per) * head_dim:(head % per + 1) * head_dim]

    query_body(head_dim, x_ref, weights, cos_ref, sin_ref, q_ref)


def query_far_kernel(head_dim, group_ref, x_ref, *rest):
    pieces, (cos_ref, sin_ref, q_ref, w_scr, sems) = rest[:NUM_FAR], rest[NUM_FAR:]
    span = x_ref.shape[-1]

    @pl.when(pl.program_id(0) == 0)
    def _():
        load_parts(pieces, w_scr, sems, far_offsets(group_ref, span))

    per = w_scr.shape[1] // head_dim

    def weights(head):
        s = head // per
        return w_scr[s * span:(s + 1) * span, (head % per) * head_dim:(head % per + 1) * head_dim]

    query_body(head_dim, x_ref, weights, cos_ref, sin_ref, q_ref)


def query_call(x, weights, cos, sin, head_dim, group=None):
    nb, rows, d = x.shape
    width = weights[0].shape[1]
    heads = 2 * width // head_dim
    step = ROW_BLOCK // rows
    full = lambda *shape: pl.BlockSpec(shape, lambda i: (0,) * len(shape))
    x_spec = pl.BlockSpec((step, rows, d), lambda i: (i, 0, 0))
    tabs = [full(rows, head_dim // 2)] * 2
    if group is None:
        kernel, specs, args, scratch = query_near_kernel, [x_spec] + [full(d, width)] * 2 + tabs, (x, *weights, cos, sin), []
    else:
        kernel, specs, args = query_far_kernel, [SMEM, x_spec] + [ANY] * NUM_FAR + tabs, (group, x, *weights, cos, sin)
        scratch = [pltpu.VMEM((2 * d, width), jnp.bfloat16), pltpu.SemaphoreType.DMA((NUM_FAR,))]
    return pl.pallas_call(
        functools.partial(kernel, head_dim),
        grid=(nb // step,),
        in_specs=specs,
        out_specs=pl.BlockSpec((step, heads, rows, head_dim), lambda i: (i, 0, 0, 0)),
        out_shape=jax.ShapeDtypeStruct((nb, heads, rows, head_dim), jnp.bfloat16),
        scratch_shapes=scratch,
        compiler_params=params(VMEM_LIMIT),
        cost_estimate=cost(4 * nb * rows * d * width, 2 * nb * rows * d),
        name="query_near" if group is None else "query_far",
    )(*args)


def attn_kernel(pos_ref, group_ref, pre_ref, val_ref, qa_ref, qb_ref, *rest):
    kva, kvb, h_ref, weights, gain_ref, mid_a, mid_b, x_a, x_b, k_scr, v_scr, o_scr, mid_scr, x_scr, w_scr, sems = (
        rest[:4], rest[4:8], rest[8], rest[9:9 + NUM_WO], *rest[9 + NUM_WO:])
    nb, heads, rows, hd = qa_ref.shape
    step = pl.program_id(0)
    half = pl.num_programs(0) // 2
    wide = weights[0].shape[0]
    d = h_ref.shape[-1]

    @pl.when(step == 0)
    def _():
        offs = [0, wide] + [2 * wide + o for o in far_offsets(group_ref, wide)]
        load_parts(weights, w_scr, sems, offs)

    for cond, kvs in ((step < half, kva), (step >= half, kvb)):
        @pl.when(cond)
        def _():
            for p, kv_ref in enumerate(kvs):
                k_scr[:, p * rows:(p + 1) * rows] = kv_ref[:, :, :hd]
                v_scr[:, p * rows:(p + 1) * rows] = kv_ref[:, :, hd:]

    seq = 4 * rows
    col = lax.broadcasted_iota(jnp.int32, (rows, seq), 1)
    row = lax.broadcasted_iota(jnp.int32, (rows, seq), 0) + pos_ref[0]
    start = jnp.full((rows, seq), pos_ref[0], jnp.int32)
    for p in range(1, 4):
        start = jnp.where(col >= p * rows, pos_ref[p] - p * rows, start)
    col = col + start
    gain = 1.0 + gain_ref[...].astype(jnp.float32)
    pair = 2
    for b in range(nb):
        sample = step * nb + b
        allowed = (col < val_ref[sample]) & ((col < pre_ref[sample]) | (col <= row))
        bias = jnp.where(allowed, 0.0, MASK_FILL).astype(jnp.float32)[None]
        keys, vals = k_scr[b], v_scr[b]
        head = 0
        for q_ref in (qa_ref, qb_ref):
            for g in range(0, heads, 2):
                q = q_ref[b, g:g + 2].reshape(2 * rows, hd)
                s = lax.dot_general(q, keys, (((1,), (1,)), ((), ())), preferred_element_type=jnp.float32)
                s = jnp.where(bias < 0.0, MASK_FILL, s.reshape(2, rows, seq))
                e = jnp.exp(s - jnp.max(s, axis=-1, keepdims=True))
                pr = (e * (1.0 / jnp.sum(e, axis=-1, keepdims=True))).astype(jnp.bfloat16)
                o = fdot(pr.reshape(2 * rows, seq), vals).astype(jnp.bfloat16)
                for i in range(2):
                    o_scr[b * rows:(b + 1) * rows, (head + i) * hd:(head + i + 1) * hd] = o[i * rows:(i + 1) * rows]
                head += 2
        if b % pair == pair - 1:
            lo = (b + 1 - pair) * rows
            sl = slice(lo, lo + pair * rows)
            total = fdot(o_scr[sl], w_scr[...])
            res = h_ref[b + 1 - pair:b + 1].reshape(pair * rows, d).astype(jnp.float32)
            mid = (res + total.astype(jnp.bfloat16).astype(jnp.float32)).astype(jnp.bfloat16)
            mid_scr[sl] = mid
            x_scr[sl] = norm_rows(mid.astype(jnp.float32), gain)

    for cond, mid_ref, x_ref in ((step < half, mid_a, x_a), (step >= half, mid_b, x_b)):
        @pl.when(cond)
        def _():
            mid_ref[...] = mid_scr[...]
            x_ref[...] = x_scr[...]


def attn_call(pos, group, prefix_len, valid_len, qa, qb, kv_a, kv_b, hidden, weights, gain):
    nb, heads, rows, hd = qa.shape
    d = 2 * heads * hd
    step = ROW_BLOCK // rows
    steps = nb // step
    half = steps // 2
    first, second = lambda i: jnp.minimum(i, half - 1), lambda i: jnp.maximum(i - half, 0)
    q_spec = pl.BlockSpec((step, heads, rows, hd), lambda i: (i, 0, 0, 0))
    kv_specs = [pl.BlockSpec((step, rows, 2 * hd), lambda i, f=f: (f(i), 0, 0)) for f in (first,) * 4 + (second,) * 4]
    res_specs = [pl.BlockSpec((ROW_BLOCK, d), lambda i, f=f: (f(i), 0)) for f in (first, second, first, second)]
    rows_half = nb * rows // 2
    seq = 4 * rows
    return pl.pallas_call(
        attn_kernel,
        grid=(steps,),
        in_specs=[SMEM] * 4 + [q_spec] * 2 + kv_specs + [pl.BlockSpec((step, rows, d), lambda i: (i, 0, 0))] + [ANY] * NUM_WO
        + [pl.BlockSpec((1, d), lambda i: (0, 0))],
        out_specs=res_specs,
        out_shape=[jax.ShapeDtypeStruct((rows_half, d), jnp.bfloat16)] * 4,
        scratch_shapes=[pltpu.VMEM((step, seq, hd), jnp.bfloat16)] * 2 + [pltpu.VMEM((ROW_BLOCK, d), jnp.bfloat16)] * 3
        + [pltpu.VMEM((d, d), jnp.bfloat16), pltpu.SemaphoreType.DMA((NUM_WO,))],
        compiler_params=params(VMEM_LIMIT),
        cost_estimate=cost(4 * nb * 2 * heads * rows * seq * hd + 2 * nb * rows * d * d, 8 * nb * rows * d),
        name="attention",
    )(pos, group, prefix_len, valid_len, qa, qb, *kv_a, *kv_b, hidden, *weights, gain)


def mlp_kernel(mode, num_x, num_sets, *refs):
    xs, refs = refs[:num_x], refs[num_x:]
    sets, refs = [refs[3 * i:3 * i + 3] for i in range(num_sets)], refs[3 * num_sets:]
    if mode in ("sum", "final"):
        part_hbm, refs = refs[0], refs[1:]
    if mode == "final":
        (mid_hbm, their_hbm), refs = refs[:2], refs[2:]
    _, out_hbm, x_ref, gb, ub, db, acc, stage, sems, sem_x, sem_in = refs[:11]
    bufs = refs[11:]
    m, _ = x_ref.shape
    tiles = sets[0][0].shape[1] // F_TILE
    steps = num_sets * tiles

    def copies(ws, t, slot):
        wg, wu, wd = ws
        cols = pl.ds(pl.multiple_of(t * F_TILE, F_TILE), F_TILE)
        return (
            pltpu.make_async_copy(wg.at[:, cols], gb.at[slot], sems.at[slot, 0]),
            pltpu.make_async_copy(wu.at[:, cols], ub.at[slot], sems.at[slot, 1]),
            pltpu.make_async_copy(wd.at[cols, :], db.at[slot], sems.at[slot, 2]),
        )

    def start(j, slot):
        for i in range(num_sets):
            @pl.when((j >= i * tiles) & (j < (i + 1) * tiles))
            def _():
                for c in copies(sets[i], j - i * tiles, slot):
                    c.start()

    offs, at = [], 0
    for ref in xs:
        offs.append(at)
        at += ref.shape[0]
    x_in = [pltpu.make_async_copy(ref, x_ref.at[pl.ds(off, ref.shape[0])], sem_x.at[i]) for i, (ref, off) in enumerate(zip(xs, offs))]
    for c in x_in:
        c.start()
    start(jnp.int32(0), 0)
    extra = []
    if mode in ("sum", "final"):
        row0 = part_hbm.shape[0] - m if mode == "sum" else 0
        extra.append(pltpu.make_async_copy(part_hbm.at[pl.ds(row0, m)], bufs[0], sem_in.at[0]))
    if mode == "final":
        extra.append(pltpu.make_async_copy(mid_hbm, stage, sem_in.at[1]))
        extra.append(pltpu.make_async_copy(their_hbm, bufs[1], sem_in.at[2]))
    acc[...] = jnp.zeros_like(acc)
    for c in x_in:
        c.wait()
    for c in extra:
        c.start()
    group = 2 * ROW_BLOCK

    def body(j, carry):
        slot = lax.rem(j, 2)

        @pl.when(j + 1 < steps)
        def _():
            start(j + 1, 1 - slot)

        wait_g, wait_u, wait_d = copies(sets[0], 0, slot)
        wait_g.wait()
        wait_u.wait()
        if m != group:
            wait_d.wait()

        def rows(r0):
            acts = []
            for r in range(0, group, ROW_BLOCK):
                x = x_ref[pl.ds(r0 + r, ROW_BLOCK)]
                g = fdot(x, gb[slot])
                u = fdot(x, ub[slot])
                t = jnp.tanh(g * (GELU_A + GELU_B * (g * g)))
                acts.append((g * (0.5 + 0.5 * t) * u).astype(jnp.bfloat16))
            if m == group and SPLIT_WAIT:
                wait_d.wait()
            for i, r in enumerate(range(0, group, ROW_BLOCK)):
                acc[pl.ds(r0 + r, ROW_BLOCK)] += fdot(acts[i], db[slot])

        if m == group and not SPLIT_WAIT:
            wait_d.wait()

        if m == group:
            rows(0)
        else:
            @pl.loop(0, m // group)
            def _(i):
                rows(pl.multiple_of(i * group, group))
        return carry

    lax.fori_loop(0, steps, body, 0)
    for c in extra:
        c.wait()
    chunk = ROW_BLOCK // 2
    done = []
    for i, r in enumerate(range(0, m, chunk)):
        sl = pl.ds(r, chunk)
        total = acc[sl]
        if mode in ("sum", "final"):
            total = total + bufs[0][sl].astype(jnp.float32)
        if mode == "final":
            total = (total + bufs[1][sl].astype(jnp.float32)).astype(jnp.bfloat16).astype(jnp.float32)
            total = stage[sl].astype(jnp.float32) + total
        stage[sl] = total.astype(jnp.bfloat16)
        c = pltpu.make_async_copy(stage.at[sl], out_hbm.at[pl.ds(r, chunk)], sem_x.at[i])
        c.start()
        done.append(c)
    for c in done:
        c.wait()


def mlp_call(mode, xs, sets, after, part=None, mid=None, their=None, out_rows=None):
    m, d = sum(x.shape[0] for x in xs), xs[0].shape[1]
    f = sets[0][0].shape[1]
    args = [*xs] + [w for ws in sets for w in ws]
    if mode in ("sum", "final"):
        args.append(part)
    if mode == "final":
        args += [mid, their]
    args.append(after)
    scratch = [pltpu.VMEM((m, d), jnp.bfloat16)]
    scratch += [pltpu.VMEM((2, d, F_TILE), jnp.bfloat16)] * 2 + [pltpu.VMEM((2, F_TILE, d), jnp.bfloat16)]
    scratch += [pltpu.VMEM((m, d), jnp.float32), pltpu.VMEM((m, d), jnp.bfloat16)]
    scratch += [pltpu.SemaphoreType.DMA((2, 3)), pltpu.SemaphoreType.DMA((16,)), pltpu.SemaphoreType.DMA((3,))]
    scratch += [pltpu.VMEM((m, d), jnp.bfloat16)] * {"part": 0, "sum": 1, "final": 2}[mode]
    return pl.pallas_call(
        functools.partial(mlp_kernel, mode, len(xs), len(sets)),
        in_specs=[ANY] * len(args),
        out_specs=ANY,
        out_shape=jax.ShapeDtypeStruct((out_rows or m, d), jnp.bfloat16),
        scratch_shapes=scratch,
        compiler_params=params(VMEM_LIMIT),
        cost_estimate=cost(6 * len(sets) * m * d * f, 6 * len(sets) * d * f),
    )(*args)


def combine_kernel(mid_ref, own_ref, their_ref, _, out_ref):
    mlp_out = (own_ref[...].astype(jnp.float32) + their_ref[...].astype(jnp.float32)).astype(jnp.bfloat16)
    out_ref[...] = (mid_ref[...].astype(jnp.float32) + mlp_out.astype(jnp.float32)).astype(jnp.bfloat16)


def combine_call(mid, own, their, out):
    m, d = mid.shape
    step = ROW_BLOCK // 2
    off = (out.shape[0] - m) // step
    blk = pl.BlockSpec((step, d), lambda i: (i, 0))
    return pl.pallas_call(
        combine_kernel,
        grid=(m // step,),
        in_specs=[blk] * 3 + [ANY],
        out_specs=pl.BlockSpec((step, d), lambda i: (i + off, 0)),
        out_shape=jax.ShapeDtypeStruct(out.shape, jnp.bfloat16),
        input_output_aliases={3: 0},
        compiler_params=params(VMEM_LIMIT),
        cost_estimate=cost(4 * m * d, 8 * m * d),
        name="combine",
    )(mid, own, their, out)


def solution(mesh):
    tp_size, dp_size = mesh.shape["tp"], mesh.shape["dp"]
    row_spec = P("dp", "tp", None)
    arg_specs = (row_spec, P("dp"), P("dp"), P(), P(None, "tp"), P(), P(), P("tp", None), P(), P(None, "tp"), P(None, "tp"), P("tp", None))

    def swap(a, axis, bit):
        return lax.ppermute(a, axis, [(i, i ^ bit) for i in range(mesh.shape[axis])])

    def spread(w, me_dp):
        size = w.shape[0] // dp_size
        quarter = lax.dynamic_slice_in_dim(w, me_dp * size, size, axis=0)
        return swap(quarter, "tp", 2)

    def gather(got):
        half = got.shape[0] // 2
        y = swap(got, "dp", 1)
        z = swap(got, "dp", 2)
        far = [got, y, z, swap(y[:half], "dp", 2), swap(z[half:], "dp", 1)]
        return far + [swap(a, "tp", 1) for a in far]

    def local_layer(hidden, prefix_len, valid_len, norm_attn, w_query, w_key, w_value, w_out, norm_mlp, w_gate, w_up, w_down):
        nb, rows, d = hidden.shape
        head_dim = w_key.shape[1]
        me, me_dp = lax.axis_index("tp"), lax.axis_index("dp")
        group = jnp.bitwise_xor(me_dp, jnp.arange(dp_size, dtype=jnp.int32))
        pos = jnp.bitwise_xor(me, jnp.arange(tp_size, dtype=jnp.int32)) * rows
        cos, sin = rope_tables(me * rows + jnp.arange(rows), head_dim)

        wq_got = spread(w_query, me_dp)
        wo_got = spread(w_out, me_dp)
        w_query_c = swap(w_query, "tp", 1)
        normed, key_local, value_local, kv_a, kv_b = kv_call(hidden, norm_attn[None], w_key, w_value, cos, sin)
        kvs = []
        for kv in (kv_a, kv_b):
            kv_x = swap(kv, "tp", 2)
            kvs.append((kv, swap(kv, "tp", 1), kv_x, swap(kv_x, "tp", 1)))
        query_a = query_call(normed, (w_query, w_query_c), cos, sin, head_dim)
        query_b = query_call(normed, gather(wq_got), cos, sin, head_dim, group)
        w_outs = [w_out, swap(w_out, "tp", 1)] + gather(wo_got)
        near = (w_gate, w_up, w_down)
        far = tuple(swap(w, "tp", 1) for w in near)

        mid_a, mid_b, x_a, x_b = attn_call(pos, group, prefix_len, valid_len, query_a, query_b, kvs[0], kvs[1], hidden, w_outs, norm_mlp[None])
        mids, mine = [mid_a, mid_b], [x_a, x_b]
        theirs = [swap(x, "tp", 2) for x in mine]

        own = mlp_call("part", mine, [near], mine[1])
        part_a = mlp_call("part", theirs[:1], [near, far], own)
        their_a = swap(part_a, "tp", 2)
        part_b = mlp_call("part", theirs[1:], [near, far], part_a)
        their_b = swap(part_b, "tp", 2)
        out = mlp_call("final", mine[:1], [far], part_b, own, mids[0], their_a, nb * rows)
        own_b = mlp_call("sum", mine[1:], [far], out, own)
        out = combine_call(mids[1], own_b, their_b, out)
        return out.reshape(nb, rows, d), key_local, value_local

    return jax.shard_map(local_layer, mesh=mesh, in_specs=arg_specs, out_specs=(row_spec, row_spec, row_spec), check_vma=False)
```

```python
import functools

import jax
import jax.numpy as jnp
from jax import lax
from jax.experimental import pallas as pl
from jax.experimental.pallas import tpu as pltpu
from jax.sharding import PartitionSpec as P


NORM_EPS = 1e-6
ROPE_BASE = 10000.0
MASK_FILL = -1e30
GELU_A = 0.7978845608028654
GELU_B = 0.7978845608028654 * 0.044715
MIB = 1024 * 1024

F_TILE = 512
ROW_BLOCK = 448

VMEM_MIB = 63


ANY = pl.BlockSpec(memory_space=pl.ANY)
SMEM = pl.BlockSpec(memory_space=pltpu.SMEM)


def params(limit_mib, **kw):
    return pltpu.CompilerParams(vmem_limit_bytes=limit_mib * MIB, **kw)


def cost(flops, nbytes):
    return pl.CostEstimate(flops=int(flops), bytes_accessed=int(nbytes), transcendentals=0)


def fdot(a, b):
    return jnp.dot(a, b, preferred_element_type=jnp.float32)


def rope_tables(positions, head_dim):
    half_dim = head_dim // 2
    inv_freq = ROPE_BASE ** (-2.0 * jnp.arange(half_dim, dtype=jnp.float32) / head_dim)
    angles = positions.astype(jnp.float32)[:, None] * inv_freq[None, :]
    return jnp.cos(angles), jnp.sin(angles)


def norm_rows(acts, gain):
    inv_rms = lax.rsqrt(jnp.mean(acts * acts, axis=-1, keepdims=True) + NORM_EPS)
    return (acts * inv_rms * gain).astype(jnp.bfloat16)


def rope_halves(vec, cos, sin):
    half = vec.shape[-1] // 2
    a, c = vec[..., :half], vec[..., half:]
    return a * cos - c * sin, c * cos + a * sin


def kv_kernel(h_ref, gain_ref, wk_ref, wv_ref, cos_ref, sin_ref, x_ref, k_ref, v_ref, kva_ref, kvb_ref):
    nb, rows, d = h_ref.shape
    gain = 1.0 + gain_ref[...].astype(jnp.float32)
    for b in range(nb):
        x_ref[b] = norm_rows(h_ref[b].astype(jnp.float32), gain)
    x = x_ref[...].reshape(nb * rows, d)
    key = fdot(x, wk_ref[...]).reshape(nb, rows, -1)
    lo, hi = rope_halves(key, cos_ref[...][None], sin_ref[...][None])
    half = lo.shape[-1]
    k_ref[:, :, :half] = lo.astype(jnp.bfloat16)
    k_ref[:, :, half:] = hi.astype(jnp.bfloat16)
    v_ref[...] = fdot(x, wv_ref[...]).astype(jnp.bfloat16).reshape(nb, rows, -1)
    first = pl.program_id(0) < pl.num_programs(0) // 2

    @pl.when(first)
    def _():
        kva_ref[:, :, :2 * half] = k_ref[...]
        kva_ref[:, :, 2 * half:] = v_ref[...]

    @pl.when(jnp.logical_not(first))
    def _():
        kvb_ref[:, :, :2 * half] = k_ref[...]
        kvb_ref[:, :, 2 * half:] = v_ref[...]


def kv_call(hidden, gain, w_key, w_value, cos, sin):
    nb, rows, d = hidden.shape
    hd = w_key.shape[1]
    step = ROW_BLOCK // rows
    steps = nb // step
    full = lambda *shape: pl.BlockSpec(shape, lambda i: (0,) * len(shape))
    blk = lambda w: pl.BlockSpec((step, rows, w), lambda i: (i, 0, 0))
    kva = pl.BlockSpec((step, rows, 2 * hd), lambda i: (jnp.minimum(i, steps // 2 - 1), 0, 0))
    kvb = pl.BlockSpec((step, rows, 2 * hd), lambda i: (jnp.maximum(i - steps // 2, 0), 0, 0))
    return pl.pallas_call(
        kv_kernel,
        grid=(steps,),
        in_specs=[blk(d), full(1, d), full(d, hd), full(d, hd), full(rows, hd // 2), full(rows, hd // 2)],
        out_specs=[blk(d), blk(hd), blk(hd), kva, kvb],
        out_shape=[jax.ShapeDtypeStruct((n, rows, w), jnp.bfloat16) for n, w in ((nb, d), (nb, hd), (nb, hd), (nb // 2, 2 * hd), (nb // 2, 2 * hd))],
        compiler_params=params(VMEM_MIB),
        cost_estimate=cost(4 * nb * rows * d * hd, 4 * nb * rows * d),
        name="kv_proj",
    )(hidden, gain, w_key, w_value, cos, sin)


def load_parts(parts, dst, sems, offsets):
    for i, (ref, off) in enumerate(zip(parts, offsets)):
        pltpu.make_async_copy(ref, dst.at[pl.ds(off, ref.shape[0])], sems.at[i]).start()
    for i, (ref, off) in enumerate(zip(parts, offsets)):
        pltpu.make_async_copy(ref, dst.at[pl.ds(off, ref.shape[0])], sems.at[i]).wait()


def query_body(head_dim, x_ref, weights, cos_ref, sin_ref, q_ref):
    nb, rows, d = x_ref.shape
    x = x_ref[...].reshape(nb * rows, d)
    cos, sin = cos_ref[...][None], sin_ref[...][None]
    scale = head_dim ** -0.5
    half = head_dim // 2
    for head in range(q_ref.shape[1]):
        vec = fdot(x, weights(head)).reshape(nb, rows, head_dim)
        lo, hi = rope_halves(vec, cos, sin)
        q_ref[:, head, :, :half] = (lo * scale).astype(jnp.bfloat16)
        q_ref[:, head, :, half:] = (hi * scale).astype(jnp.bfloat16)


def query_near_kernel(head_dim, x_ref, w0_ref, w1_ref, cos_ref, sin_ref, q_ref):
    per = w0_ref.shape[1] // head_dim

    def weights(head):
        ref = (w0_ref, w1_ref)[head // per]
        return ref[:, (head % per) * head_dim:(head % per + 1) * head_dim]

    query_body(head_dim, x_ref, weights, cos_ref, sin_ref, q_ref)


def query_far_kernel(head_dim, group_ref, x_ref, *rest):
    pieces, (cos_ref, sin_ref, q_ref, w_scr, sems) = rest[:8], rest[8:]
    size = pieces[0].shape[0]
    span = 4 * size

    @pl.when(pl.program_id(0) == 0)
    def _():
        offs = [pl.multiple_of(group_ref[k] * size, size) + s * span for s in range(2) for k in range(4)]
        load_parts(pieces, w_scr, sems, offs)

    per = w_scr.shape[1] // head_dim

    def weights(head):
        s = head // per
        return w_scr[s * span:(s + 1) * span, (head % per) * head_dim:(head % per + 1) * head_dim]

    query_body(head_dim, x_ref, weights, cos_ref, sin_ref, q_ref)


def query_call(x, weights, cos, sin, head_dim, group=None):
    nb, rows, d = x.shape
    width = weights[0].shape[1]
    heads = 2 * width // head_dim
    step = ROW_BLOCK // rows
    full = lambda *shape: pl.BlockSpec(shape, lambda i: (0,) * len(shape))
    x_spec = pl.BlockSpec((step, rows, d), lambda i: (i, 0, 0))
    tabs = [full(rows, head_dim // 2)] * 2
    if group is None:
        kernel, specs, args, scratch = query_near_kernel, [x_spec] + [full(d, width)] * 2 + tabs, (x, *weights, cos, sin), []
    else:
        kernel, specs, args = query_far_kernel, [SMEM, x_spec] + [ANY] * 8 + tabs, (group, x, *weights, cos, sin)
        scratch = [pltpu.VMEM((2 * d, width), jnp.bfloat16), pltpu.SemaphoreType.DMA((8,))]
    return pl.pallas_call(
        functools.partial(kernel, head_dim),
        grid=(nb // step,),
        in_specs=specs,
        out_specs=pl.BlockSpec((step, heads, rows, head_dim), lambda i: (i, 0, 0, 0)),
        out_shape=jax.ShapeDtypeStruct((nb, heads, rows, head_dim), jnp.bfloat16),
        scratch_shapes=scratch,
        compiler_params=params(VMEM_MIB),
        cost_estimate=cost(4 * nb * rows * d * width, 2 * nb * rows * d),
        name="query_near" if group is None else "query_far",
    )(*args)


def attn_kernel(base, pos_ref, pre_ref, val_ref, qa_ref, qb_ref, kv0, kv1, kv2, kv3, o_ref, k_scr, v_scr):
    _, heads, rows, hd = qa_ref.shape
    b = pl.program_id(0) + base
    for p, kv_ref in enumerate((kv0, kv1, kv2, kv3)):
        k_scr[p * rows:(p + 1) * rows] = kv_ref[0, :, :hd]
        v_scr[p * rows:(p + 1) * rows] = kv_ref[0, :, hd:]
    seq = 4 * rows
    col = lax.broadcasted_iota(jnp.int32, (rows, seq), 1)
    row = lax.broadcasted_iota(jnp.int32, (rows, seq), 0) + pos_ref[0]
    start = jnp.full((rows, seq), pos_ref[0], jnp.int32)
    for p in range(1, 4):
        start = jnp.where(col >= p * rows, pos_ref[p] - p * rows, start)
    col = col + start
    allowed = (col < val_ref[b]) & ((col < pre_ref[b]) | (col <= row))
    bias = jnp.where(allowed, 0.0, MASK_FILL).astype(jnp.float32)[None]
    keys, vals = k_scr[...], v_scr[...]
    head = 0
    for q_ref in (qa_ref, qb_ref):
        for g in range(0, heads, 2):
            q = q_ref[0, g:g + 2].reshape(2 * rows, hd)
            s = lax.dot_general(q, keys, (((1,), (1,)), ((), ())), preferred_element_type=jnp.float32)
            s = jnp.where(bias < 0.0, MASK_FILL, s.reshape(2, rows, seq))
            e = jnp.exp(s - jnp.max(s, axis=-1, keepdims=True))
            pr = (e * (1.0 / jnp.sum(e, axis=-1, keepdims=True))).astype(jnp.bfloat16)
            o = fdot(pr.reshape(2 * rows, seq), vals).astype(jnp.bfloat16)
            for i in range(2):
                o_ref[0, :, (head + i) * hd:(head + i + 1) * hd] = o[i * rows:(i + 1) * rows]
            head += 2


def attn_call(base, count, pos, prefix_len, valid_len, qa, qb, kvs):
    _, heads, rows, hd = qa.shape
    d = 2 * heads * hd
    q_spec = pl.BlockSpec((1, heads, rows, hd), lambda i: (i + base, 0, 0, 0))
    kv_spec = pl.BlockSpec((1, rows, 2 * hd), lambda i: (i, 0, 0))
    return pl.pallas_call(
        functools.partial(attn_kernel, base),
        grid=(count,),
        in_specs=[SMEM] * 3 + [q_spec] * 2 + [kv_spec] * 4,
        out_specs=pl.BlockSpec((1, rows, d), lambda i: (i, 0, 0)),
        out_shape=jax.ShapeDtypeStruct((count, rows, d), jnp.bfloat16),
        scratch_shapes=[pltpu.VMEM((4 * rows, hd), jnp.bfloat16)] * 2,
        compiler_params=params(VMEM_MIB),
        cost_estimate=cost(4 * count * 2 * heads * rows * 4 * rows * hd * 2, 8 * count * rows * d),
        name="attention",
    )(pos, prefix_len, valid_len, qa, qb, *kvs)


def out_kernel(group_ref, o_ref, h_ref, *rest):
    weights, gain_ref, mid_ref, x_ref, w_scr, sems = rest[:10], *rest[10:]
    nb, rows, d = o_ref.shape
    wide, size = weights[0].shape[0], weights[2].shape[0]

    @pl.when(pl.program_id(0) == 0)
    def _():
        offs = [0, wide] + [pl.multiple_of(group_ref[k] * size, size) + s * wide for s in (2, 3) for k in range(4)]
        load_parts(weights, w_scr, sems, offs)

    gain = 1.0 + gain_ref[...].astype(jnp.float32)
    pair = 2
    for b in range(0, nb, pair):
        total = fdot(o_ref[b:b + pair].reshape(pair * rows, d), w_scr[...])
        res = h_ref[b:b + pair].reshape(pair * rows, d).astype(jnp.float32)
        mid = (res + total.astype(jnp.bfloat16).astype(jnp.float32)).astype(jnp.bfloat16)
        mid_ref[b * rows:(b + pair) * rows] = mid
        x_ref[b * rows:(b + pair) * rows] = norm_rows(mid.astype(jnp.float32), gain)


def out_call(base, o, hidden, group, weights, gain):
    count, rows, d = o.shape
    step = ROW_BLOCK // rows
    off = base // step
    full = lambda *shape: pl.BlockSpec(shape, lambda i: (0,) * len(shape))
    res_spec = pl.BlockSpec((ROW_BLOCK, d), lambda i: (i, 0))
    return pl.pallas_call(
        out_kernel,
        grid=(count // step,),
        in_specs=[SMEM, pl.BlockSpec((step, rows, d), lambda i: (i, 0, 0)),
                  pl.BlockSpec((step, rows, d), lambda i: (i + off, 0, 0))]
        + [ANY] * 10 + [full(1, d)],
        out_specs=[res_spec, res_spec],
        out_shape=[jax.ShapeDtypeStruct((count * rows, d), jnp.bfloat16)] * 2,
        scratch_shapes=[pltpu.VMEM((d, d), jnp.bfloat16), pltpu.SemaphoreType.DMA((10,))],
        compiler_params=params(VMEM_MIB),
        cost_estimate=cost(2 * count * rows * d * d, 8 * count * rows * d),
        name="out_proj",
    )(group, o, hidden, *weights, gain)


def mlp_kernel(xa_hbm, xb_hbm, mid_a, mid_b, wg0, wu0, wd0, out_hbm, wg1, wu1, wd1, in_a, in_b, send_a, send_b, ret_a, ret_b,
               xbuf, own, acc, stage, mid, their, gb, ub, db, sems, sem_x, sem_in, sem_out, far_send, far_recv, row_send, row_recv):
    m, _ = xa_hbm.shape
    tiles = wg0.shape[1] // F_TILE
    steps = 8 * tiles
    starts = (0, tiles, 2 * tiles, 4 * tiles, 6 * tiles, 7 * tiles)
    me = lax.axis_index("tp")
    size = lax.axis_size("tp")
    chip = lax.rem(me + size // 2, size)
    core = me + 1 - 2 * lax.rem(me, 2)

    barrier = pltpu.get_barrier_semaphore()
    for peer in (chip, core):
        pl.semaphore_signal(barrier, inc=1, device_id={"tp": peer}, device_id_type=pl.DeviceIdType.MESH)
    pl.semaphore_wait(barrier, 2)

    def remote(src, dst, ssem, rsem, peer):
        return pltpu.make_async_remote_copy(src_ref=src, dst_ref=dst, send_sem=ssem, recv_sem=rsem,
                                            device_id={"tp": peer}, device_id_type=pl.DeviceIdType.MESH)

    rows = [remote(src, dst, row_send.at[i], row_recv.at[i], chip)
            for i, (src, dst) in enumerate(((xa_hbm, in_a), (xb_hbm, in_b), (send_a, ret_a), (send_b, ret_b)))]
    far = [remote(src, dst, far_send.at[i], far_recv.at[i], core)
           for i, (src, dst) in enumerate(((wg0, wg1), (wu0, wu1), (wd0, wd1)))]
    rows[0].start()
    for c in far:
        c.start()

    def tile_copies(ws, t, slot):
        wg, wu, wd = ws
        cols = pl.ds(pl.multiple_of(t * F_TILE, F_TILE), F_TILE)
        return (
            pltpu.make_async_copy(wg.at[:, cols], gb.at[slot], sems.at[slot, 0]),
            pltpu.make_async_copy(wu.at[:, cols], ub.at[slot], sems.at[slot, 1]),
            pltpu.make_async_copy(wd.at[cols, :], db.at[slot], sems.at[slot, 2]),
        )

    def between(j, lo, hi):
        return (j >= lo * tiles) & (j < hi * tiles)

    def start(j, slot):
        use_far = between(j, 3, 4) | between(j, 5, 8)
        t = lax.rem(j, tiles)

        @pl.when(jnp.logical_not(use_far))
        def _():
            for c in tile_copies((wg0, wu0, wd0), t, slot):
                c.start()

        @pl.when(use_far)
        def _():
            for c in tile_copies((wg1, wu1, wd1), t, slot):
                c.start()

    def x_copy(src, slot):
        return pltpu.make_async_copy(src, xbuf.at[slot], sem_x.at[slot])

    x_copy(xa_hbm, 0).start()
    start(jnp.int32(0), 0)
    acc[...] = jnp.zeros_like(acc)
    x_sources = (xa_hbm, xb_hbm, in_a, in_b, xa_hbm, xb_hbm)
    chunk = ROW_BLOCK // 2

    def chunks(fn):
        @pl.loop(0, m // chunk)
        def _(i):
            fn(pl.ds(pl.multiple_of(i * chunk, chunk), chunk))

    def body(j, carry):
        slot = lax.rem(j, 2)

        @pl.when(j == 2 * tiles - 4)
        def _():
            rows[1].start()

        @pl.when(j == 3 * tiles - 2)
        def _():
            for c in far:
                c.wait_recv()

        for k in range(1, 6):
            @pl.when(j == starts[k] - 2)
            def _():
                if k in (2, 3):
                    rows[k - 2].wait_recv()
                x_copy(x_sources[k], k % 2).start()

        for k in (4, 5):
            @pl.when(j == starts[k] + tiles - 3)
            def _():
                pltpu.make_async_copy((mid_a, mid_b)[k - 4], mid, sem_in.at[0]).start()

        for k in (2, 3):
            @pl.when(j == starts[k + 1] + 1)
            def _():
                pltpu.make_async_copy(stage, (send_a, send_b)[k - 2], sem_out.at[0]).wait()
                rows[k].start()

        for k in range(6):
            @pl.when(j == starts[k])
            def _():
                x_copy(x_sources[k], k % 2).wait()

        @pl.when(j + 1 < steps)
        def _():
            start(j + 1, 1 - slot)

        for c in tile_copies((wg0, wu0, wd0), 0, slot):
            c.wait()

        first = j == starts[0]
        odd = jnp.int32(0)
        for k in range(1, 6):
            first = first | (j == starts[k])
            odd = odd + (j >= starts[k]).astype(jnp.int32)
        odd = lax.rem(odd, 2)
        acts = []
        for r in range(0, m, ROW_BLOCK):
            x = xbuf[odd, r:r + ROW_BLOCK]
            g = fdot(x, gb[slot])
            u = fdot(x, ub[slot])
            t = jnp.tanh(g * (GELU_A + GELU_B * (g * g)))
            acts.append((g * (0.5 + 0.5 * t) * u).astype(jnp.bfloat16))
        for i, r in enumerate(range(0, m, ROW_BLOCK)):
            acc[r:r + ROW_BLOCK] = jnp.where(first, 0.0, acc[r:r + ROW_BLOCK]) + fdot(acts[i], db[slot])

        for k in (0, 1):
            @pl.when(j == starts[k + 1] - 1)
            def _():
                def keep(sl):
                    own[k, sl] = acc[sl].astype(jnp.bfloat16)

                chunks(keep)

        for k in (2, 3):
            @pl.when(j == starts[k + 1] - 1)
            def _():
                def put(sl):
                    stage[sl] = acc[sl].astype(jnp.bfloat16)

                chunks(put)
                pltpu.make_async_copy(stage, (send_a, send_b)[k - 2], sem_out.at[0]).start()

        for k in (4, 5):
            @pl.when(j == starts[k] + tiles - 1)
            def _():
                ret, mid_hbm = ((ret_a, mid_a), (ret_b, mid_b))[k - 4]
                rows[k - 2].wait_recv()
                got = pltpu.make_async_copy(ret, their, sem_in.at[1])
                got.start()
                pltpu.make_async_copy(mid_hbm, mid, sem_in.at[0]).wait()
                got.wait()
                if k == 5:
                    pltpu.make_async_copy(stage, out_hbm.at[pl.ds(0, m)], sem_out.at[1]).wait()

                def finish(sl):
                    total = acc[sl] + own[k - 4, sl].astype(jnp.float32) + their[sl].astype(jnp.float32)
                    stage[sl] = (mid[sl].astype(jnp.float32) + total.astype(jnp.bfloat16).astype(jnp.float32)).astype(jnp.bfloat16)

                chunks(finish)
                pltpu.make_async_copy(stage, out_hbm.at[pl.ds((k - 4) * m, m)], sem_out.at[k - 3]).start()
        return carry

    lax.fori_loop(0, steps, body, 0)
    pltpu.make_async_copy(stage, out_hbm.at[pl.ds(m, m)], sem_out.at[2]).wait()
    for c in rows + far:
        c.wait_send()


def mlp_call(x_a, x_b, mid_a, mid_b, weights):
    m, d = x_a.shape
    f = weights[0].shape[1]
    half = jax.ShapeDtypeStruct((m, d), jnp.bfloat16)
    outs = [jax.ShapeDtypeStruct((2 * m, d), jnp.bfloat16)] + [jax.ShapeDtypeStruct(w.shape, w.dtype) for w in weights] + [half] * 6
    dma = pltpu.SemaphoreType.DMA
    return pl.pallas_call(
        mlp_kernel,
        in_specs=[ANY] * 7,
        out_specs=[ANY] * len(outs),
        out_shape=outs,
        scratch_shapes=[
            pltpu.VMEM((2, m, d), jnp.bfloat16), pltpu.VMEM((2, m, d), jnp.bfloat16), pltpu.VMEM((m, d), jnp.float32),
            pltpu.VMEM((m, d), jnp.bfloat16), pltpu.VMEM((m, d), jnp.bfloat16), pltpu.VMEM((m, d), jnp.bfloat16),
            pltpu.VMEM((2, d, F_TILE), jnp.bfloat16), pltpu.VMEM((2, d, F_TILE), jnp.bfloat16), pltpu.VMEM((2, F_TILE, d), jnp.bfloat16),
            dma((2, 3)), dma((2,)), dma((2,)), dma((3,)), dma((3,)), dma((3,)), dma((4,)), dma((4,)),
        ],
        compiler_params=params(60, collective_id=0, has_side_effects=True),
        cost_estimate=cost(48 * m * d * f, 48 * d * f),
        name="mlp",
    )(x_a, x_b, mid_a, mid_b, *weights)[0]


def solution(mesh):
    tp_size, dp_size = mesh.shape["tp"], mesh.shape["dp"]
    row_spec = P("dp", "tp", None)
    arg_specs = (row_spec, P("dp"), P("dp"), P(), P(None, "tp"), P(), P(), P("tp", None), P(), P(None, "tp"), P(None, "tp"), P("tp", None))

    def swap(a, axis, bit):
        return lax.ppermute(a, axis, [(i, i ^ bit) for i in range(mesh.shape[axis])])

    def spread(w, me_dp):
        size = w.shape[0] // dp_size
        quarter = lax.dynamic_slice_in_dim(w, me_dp * size, size, axis=0)
        return swap(quarter, "tp", 2)

    def gather(got, diag_first):
        y = swap(got, "dp", 1)
        z = swap(got, "dp", 2)
        diag = swap(y, "dp", 2) if diag_first else swap(z, "dp", 1)
        far = [got, y, z, diag]
        return far + [swap(a, "tp", 1) for a in far]

    def local_layer(hidden, prefix_len, valid_len, norm_attn, w_query, w_key, w_value, w_out, norm_mlp, w_gate, w_up, w_down):
        nb, rows, d = hidden.shape
        head_dim = w_key.shape[1]
        half = nb // 2
        me, me_dp = lax.axis_index("tp"), lax.axis_index("dp")
        group = jnp.bitwise_xor(me_dp, jnp.arange(dp_size, dtype=jnp.int32))
        pos = jnp.bitwise_xor(me, jnp.arange(tp_size, dtype=jnp.int32)) * rows
        cos, sin = rope_tables(me * rows + jnp.arange(rows), head_dim)

        wq_got = spread(w_query, me_dp)
        wo_got = spread(w_out, me_dp)
        w_query_c = swap(w_query, "tp", 1)
        normed, key_local, value_local, kv_a, kv_b = kv_call(hidden, norm_attn[None], w_key, w_value, cos, sin)
        kvs = []
        for kv in (kv_a, kv_b):
            kv_x = swap(kv, "tp", 2)
            kvs.append((kv, swap(kv, "tp", 1), kv_x, swap(kv_x, "tp", 1)))
        query_a = query_call(normed, (w_query, w_query_c), cos, sin, head_dim)
        query_b = query_call(normed, gather(wq_got, True), cos, sin, head_dim, group)
        w_outs = [w_out, swap(w_out, "tp", 1)] + gather(wo_got, False)
        near = (w_gate, w_up, w_down)

        mids, mine = [], []
        for base, kv in ((0, kvs[0]), (half, kvs[1])):
            o = attn_call(base, half, pos, prefix_len, valid_len, query_a, query_b, kv)
            mid, x = out_call(base, o, hidden, group, w_outs, norm_mlp[None])
            mids.append(mid)
            mine.append(x)
        out = mlp_call(*mine, *mids, near)
        return out.reshape(nb, rows, d), key_local, value_local

    return jax.shard_map(local_layer, mesh=mesh, in_specs=arg_specs, out_specs=(row_spec, row_spec, row_spec), check_vma=False)
```

```python
import functools

import jax
import jax.numpy as jnp
from jax import lax
from jax.experimental import pallas as pl
from jax.experimental.pallas import tpu as pltpu
from jax.sharding import PartitionSpec as P


NORM_EPS = 1e-6
ROPE_BASE = 10000.0
MASK_FILL = -1e30
GELU_A = 0.7978845608028654
GELU_B = 0.7978845608028654 * 0.044715
MIB = 1024 * 1024

F_TILE = 512
ROW_BLOCK = 448

VMEM_MIB = 63


ANY = pl.BlockSpec(memory_space=pl.ANY)
SMEM = pl.BlockSpec(memory_space=pltpu.SMEM)


def params(limit_mib, **kw):
    return pltpu.CompilerParams(vmem_limit_bytes=limit_mib * MIB, **kw)


def cost(flops, nbytes):
    return pl.CostEstimate(flops=int(flops), bytes_accessed=int(nbytes), transcendentals=0)


def fdot(a, b):
    return jnp.dot(a, b, preferred_element_type=jnp.float32)


def rope_tables(positions, head_dim):
    half_dim = head_dim // 2
    inv_freq = ROPE_BASE ** (-2.0 * jnp.arange(half_dim, dtype=jnp.float32) / head_dim)
    angles = positions.astype(jnp.float32)[:, None] * inv_freq[None, :]
    return jnp.cos(angles), jnp.sin(angles)


def norm_rows(acts, gain):
    inv_rms = lax.rsqrt(jnp.mean(acts * acts, axis=-1, keepdims=True) + NORM_EPS)
    return (acts * inv_rms * gain).astype(jnp.bfloat16)


def rope_halves(vec, cos, sin):
    half = vec.shape[-1] // 2
    a, c = vec[..., :half], vec[..., half:]
    return a * cos - c * sin, c * cos + a * sin


def kv_kernel(h_ref, gain_ref, wk_ref, wv_ref, cos_ref, sin_ref, x_ref, k_ref, v_ref, kva_ref, kvb_ref):
    nb, rows, d = h_ref.shape
    gain = 1.0 + gain_ref[...].astype(jnp.float32)
    for b in range(nb):
        x_ref[b] = norm_rows(h_ref[b].astype(jnp.float32), gain)
    x = x_ref[...].reshape(nb * rows, d)
    key = fdot(x, wk_ref[...]).reshape(nb, rows, -1)
    lo, hi = rope_halves(key, cos_ref[...][None], sin_ref[...][None])
    half = lo.shape[-1]
    k_ref[:, :, :half] = lo.astype(jnp.bfloat16)
    k_ref[:, :, half:] = hi.astype(jnp.bfloat16)
    v_ref[...] = fdot(x, wv_ref[...]).astype(jnp.bfloat16).reshape(nb, rows, -1)
    first = pl.program_id(0) < pl.num_programs(0) // 2

    @pl.when(first)
    def _():
        kva_ref[:, :, :2 * half] = k_ref[...]
        kva_ref[:, :, 2 * half:] = v_ref[...]

    @pl.when(jnp.logical_not(first))
    def _():
        kvb_ref[:, :, :2 * half] = k_ref[...]
        kvb_ref[:, :, 2 * half:] = v_ref[...]


def kv_call(hidden, gain, w_key, w_value, cos, sin):
    nb, rows, d = hidden.shape
    hd = w_key.shape[1]
    step = ROW_BLOCK // rows
    steps = nb // step
    full = lambda *shape: pl.BlockSpec(shape, lambda i: (0,) * len(shape))
    blk = lambda w: pl.BlockSpec((step, rows, w), lambda i: (i, 0, 0))
    kva = pl.BlockSpec((step, rows, 2 * hd), lambda i: (jnp.minimum(i, steps // 2 - 1), 0, 0))
    kvb = pl.BlockSpec((step, rows, 2 * hd), lambda i: (jnp.maximum(i - steps // 2, 0), 0, 0))
    return pl.pallas_call(
        kv_kernel,
        grid=(steps,),
        in_specs=[blk(d), full(1, d), full(d, hd), full(d, hd), full(rows, hd // 2), full(rows, hd // 2)],
        out_specs=[blk(d), blk(hd), blk(hd), kva, kvb],
        out_shape=[jax.ShapeDtypeStruct((n, rows, w), jnp.bfloat16) for n, w in ((nb, d), (nb, hd), (nb, hd), (nb // 2, 2 * hd), (nb // 2, 2 * hd))],
        compiler_params=params(VMEM_MIB),
        cost_estimate=cost(4 * nb * rows * d * hd, 4 * nb * rows * d),
        name="kv_proj",
    )(hidden, gain, w_key, w_value, cos, sin)


def load_parts(parts, dst, sems, offsets):
    for i, (ref, off) in enumerate(zip(parts, offsets)):
        pltpu.make_async_copy(ref, dst.at[pl.ds(off, ref.shape[0])], sems.at[i]).start()
    for i, (ref, off) in enumerate(zip(parts, offsets)):
        pltpu.make_async_copy(ref, dst.at[pl.ds(off, ref.shape[0])], sems.at[i]).wait()


def query_body(head_dim, x_ref, weights, cos_ref, sin_ref, q_ref):
    nb, rows, d = x_ref.shape
    x = x_ref[...].reshape(nb * rows, d)
    cos, sin = cos_ref[...][None], sin_ref[...][None]
    scale = head_dim ** -0.5
    half = head_dim // 2
    for head in range(q_ref.shape[1]):
        vec = fdot(x, weights(head)).reshape(nb, rows, head_dim)
        lo, hi = rope_halves(vec, cos, sin)
        q_ref[:, head, :, :half] = (lo * scale).astype(jnp.bfloat16)
        q_ref[:, head, :, half:] = (hi * scale).astype(jnp.bfloat16)


def query_near_kernel(head_dim, x_ref, w0_ref, w1_ref, cos_ref, sin_ref, q_ref):
    per = w0_ref.shape[1] // head_dim

    def weights(head):
        ref = (w0_ref, w1_ref)[head // per]
        return ref[:, (head % per) * head_dim:(head % per + 1) * head_dim]

    query_body(head_dim, x_ref, weights, cos_ref, sin_ref, q_ref)


def query_far_kernel(head_dim, group_ref, x_ref, *rest):
    pieces, (cos_ref, sin_ref, q_ref, w_scr, sems) = rest[:8], rest[8:]
    size = pieces[0].shape[0]
    span = 4 * size

    @pl.when(pl.program_id(0) == 0)
    def _():
        offs = [pl.multiple_of(group_ref[k] * size, size) + s * span for s in range(2) for k in range(4)]
        load_parts(pieces, w_scr, sems, offs)

    per = w_scr.shape[1] // head_dim

    def weights(head):
        s = head // per
        return w_scr[s * span:(s + 1) * span, (head % per) * head_dim:(head % per + 1) * head_dim]

    query_body(head_dim, x_ref, weights, cos_ref, sin_ref, q_ref)


def query_call(x, weights, cos, sin, head_dim, group=None):
    nb, rows, d = x.shape
    width = weights[0].shape[1]
    heads = 2 * width // head_dim
    step = ROW_BLOCK // rows
    full = lambda *shape: pl.BlockSpec(shape, lambda i: (0,) * len(shape))
    x_spec = pl.BlockSpec((step, rows, d), lambda i: (i, 0, 0))
    tabs = [full(rows, head_dim // 2)] * 2
    if group is None:
        kernel, specs, args, scratch = query_near_kernel, [x_spec] + [full(d, width)] * 2 + tabs, (x, *weights, cos, sin), []
    else:
        kernel, specs, args = query_far_kernel, [SMEM, x_spec] + [ANY] * 8 + tabs, (group, x, *weights, cos, sin)
        scratch = [pltpu.VMEM((2 * d, width), jnp.bfloat16), pltpu.SemaphoreType.DMA((8,))]
    return pl.pallas_call(
        functools.partial(kernel, head_dim),
        grid=(nb // step,),
        in_specs=specs,
        out_specs=pl.BlockSpec((step, heads, rows, head_dim), lambda i: (i, 0, 0, 0)),
        out_shape=jax.ShapeDtypeStruct((nb, heads, rows, head_dim), jnp.bfloat16),
        scratch_shapes=scratch,
        compiler_params=params(VMEM_MIB),
        cost_estimate=cost(4 * nb * rows * d * width, 2 * nb * rows * d),
        name="query_near" if group is None else "query_far",
    )(*args)


def attn_kernel(base, pos_ref, pre_ref, val_ref, qa_ref, qb_ref, kv0, kv1, kv2, kv3, *rest):
    o_ref, k_scr, v_scr = rest[-3:]
    _, heads, rows, hd = qa_ref.shape
    b = pl.program_id(0) + base
    for p, kv_ref in enumerate((kv0, kv1, kv2, kv3)):
        k_scr[p * rows:(p + 1) * rows] = kv_ref[0, :, :hd]
        v_scr[p * rows:(p + 1) * rows] = kv_ref[0, :, hd:]
    seq = 4 * rows
    col = lax.broadcasted_iota(jnp.int32, (rows, seq), 1)
    row = lax.broadcasted_iota(jnp.int32, (rows, seq), 0) + pos_ref[0]
    start = jnp.full((rows, seq), pos_ref[0], jnp.int32)
    for p in range(1, 4):
        start = jnp.where(col >= p * rows, pos_ref[p] - p * rows, start)
    col = col + start
    allowed = (col < val_ref[b]) & ((col < pre_ref[b]) | (col <= row))
    bias = jnp.where(allowed, 0.0, MASK_FILL).astype(jnp.float32)[None]
    keys, vals = k_scr[...], v_scr[...]
    head = 0
    for q_ref in (qa_ref, qb_ref):
        for g in range(0, heads, 2):
            q = q_ref[0, g:g + 2].reshape(2 * rows, hd)
            s = lax.dot_general(q, keys, (((1,), (1,)), ((), ())), preferred_element_type=jnp.float32)
            s = jnp.where(bias < 0.0, MASK_FILL, s.reshape(2, rows, seq))
            e = jnp.exp(s - jnp.max(s, axis=-1, keepdims=True))
            pr = (e * (1.0 / jnp.sum(e, axis=-1, keepdims=True))).astype(jnp.bfloat16)
            o = fdot(pr.reshape(2 * rows, seq), vals).astype(jnp.bfloat16)
            for i in range(2):
                o_ref[0, :, (head + i) * hd:(head + i + 1) * hd] = o[i * rows:(i + 1) * rows]
            head += 2


def attn_call(base, count, pos, prefix_len, valid_len, qa, qb, kvs, into=None):
    nb, heads, rows, hd = qa.shape
    d = 2 * heads * hd
    q_spec = pl.BlockSpec((1, heads, rows, hd), lambda i: (i + base, 0, 0, 0))
    kv_spec = pl.BlockSpec((1, rows, 2 * hd), lambda i: (i, 0, 0))
    return pl.pallas_call(
        functools.partial(attn_kernel, base),
        grid=(count,),
        in_specs=[SMEM] * 3 + [q_spec] * 2 + [kv_spec] * 4 + [ANY] * (into is not None),
        out_specs=pl.BlockSpec((1, rows, d), lambda i: (i + base, 0, 0)),
        out_shape=jax.ShapeDtypeStruct((nb, rows, d), jnp.bfloat16),
        input_output_aliases={} if into is None else {9: 0},
        scratch_shapes=[pltpu.VMEM((4 * rows, hd), jnp.bfloat16)] * 2,
        compiler_params=params(VMEM_MIB),
        cost_estimate=cost(4 * count * 2 * heads * rows * 4 * rows * hd * 2, 8 * count * rows * d),
        name="attention",
    )(pos, prefix_len, valid_len, qa, qb, *kvs, *(() if into is None else (into,)))


def out_kernel(group_ref, o_ref, h_ref, *rest):
    weights, gain_ref, mid_ref, x_ref, w_scr, sems = rest[:10], *rest[10:]
    nb, rows, d = o_ref.shape
    wide, size = weights[0].shape[0], weights[2].shape[0]

    @pl.when(pl.program_id(0) == 0)
    def _():
        offs = [0, wide] + [pl.multiple_of(group_ref[k] * size, size) + s * wide for s in (2, 3) for k in range(4)]
        load_parts(weights, w_scr, sems, offs)

    gain = 1.0 + gain_ref[...].astype(jnp.float32)
    pair = 2
    for b in range(0, nb, pair):
        total = fdot(o_ref[b:b + pair].reshape(pair * rows, d), w_scr[...])
        res = h_ref[b:b + pair].reshape(pair * rows, d).astype(jnp.float32)
        mid = (res + total.astype(jnp.bfloat16).astype(jnp.float32)).astype(jnp.bfloat16)
        mid_ref[b * rows:(b + pair) * rows] = mid
        x_ref[b * rows:(b + pair) * rows] = norm_rows(mid.astype(jnp.float32), gain)


def out_call(base, o, hidden, group, weights, gain):
    count, rows, d = o.shape
    step = ROW_BLOCK // rows
    off = base // step
    full = lambda *shape: pl.BlockSpec(shape, lambda i: (0,) * len(shape))
    res_spec = pl.BlockSpec((ROW_BLOCK, d), lambda i: (i, 0))
    return pl.pallas_call(
        out_kernel,
        grid=(count // step,),
        in_specs=[SMEM, pl.BlockSpec((step, rows, d), lambda i: (i, 0, 0)),
                  pl.BlockSpec((step, rows, d), lambda i: (i + off, 0, 0))]
        + [ANY] * 10 + [full(1, d)],
        out_specs=[res_spec, res_spec],
        out_shape=[jax.ShapeDtypeStruct((count * rows, d), jnp.bfloat16)] * 2,
        scratch_shapes=[pltpu.VMEM((d, d), jnp.bfloat16), pltpu.SemaphoreType.DMA((10,))],
        compiler_params=params(VMEM_MIB),
        cost_estimate=cost(2 * count * rows * d * d, 8 * count * rows * d),
        name="out_proj",
    )(group, o, hidden, *weights, gain)


def mlp_kernel(x_hbm, mid_hbm, wg0, wu0, wd0, out_hbm, wg1, wu1, wd1, in_a, in_b, send_a, send_b, ret_a, ret_b,
               xbuf, own, acc, stage, mid, their, gb, ub, db, sems, sem_x, sem_in, sem_out, far_send, far_recv, row_send, row_recv):
    m, _ = in_a.shape
    xa_hbm, xb_hbm = x_hbm.at[pl.ds(0, m)], x_hbm.at[pl.ds(m, m)]
    mid_a, mid_b = mid_hbm.at[pl.ds(0, m)], mid_hbm.at[pl.ds(m, m)]
    tiles = wg0.shape[1] // F_TILE
    steps = 8 * tiles
    starts = (0, tiles, 2 * tiles, 4 * tiles, 6 * tiles, 7 * tiles)
    me = lax.axis_index("tp")
    size = lax.axis_size("tp")
    chip = lax.rem(me + size // 2, size)
    core = me + 1 - 2 * lax.rem(me, 2)

    pltpu.make_async_copy(xa_hbm, xbuf.at[0], sem_x.at[0]).start()
    for ws, buf, i in ((wg0.at[:, pl.ds(0, F_TILE)], gb, 0), (wu0.at[:, pl.ds(0, F_TILE)], ub, 1), (wd0.at[pl.ds(0, F_TILE), :], db, 2)):
        pltpu.make_async_copy(ws, buf.at[0], sems.at[0, i]).start()

    barrier = pltpu.get_barrier_semaphore()
    for peer in (chip, core):
        pl.semaphore_signal(barrier, inc=1, device_id={"tp": peer}, device_id_type=pl.DeviceIdType.MESH)
    pl.semaphore_wait(barrier, 2)

    def remote(src, dst, ssem, rsem, peer):
        return pltpu.make_async_remote_copy(src_ref=src, dst_ref=dst, send_sem=ssem, recv_sem=rsem,
                                            device_id={"tp": peer}, device_id_type=pl.DeviceIdType.MESH)

    rows = [remote(src, dst, row_send.at[i], row_recv.at[i], chip)
            for i, (src, dst) in enumerate(((xa_hbm, in_a), (xb_hbm, in_b), (send_a, ret_a), (send_b, ret_b)))]
    far = [remote(src, dst, far_send.at[i], far_recv.at[i], core)
           for i, (src, dst) in enumerate(((wg0, wg1), (wu0, wu1), (wd0, wd1)))]
    rows[0].start()
    for c in far:
        c.start()

    def tile_copies(ws, t, slot):
        wg, wu, wd = ws
        cols = pl.ds(pl.multiple_of(t * F_TILE, F_TILE), F_TILE)
        return (
            pltpu.make_async_copy(wg.at[:, cols], gb.at[slot], sems.at[slot, 0]),
            pltpu.make_async_copy(wu.at[:, cols], ub.at[slot], sems.at[slot, 1]),
            pltpu.make_async_copy(wd.at[cols, :], db.at[slot], sems.at[slot, 2]),
        )

    def between(j, lo, hi):
        return (j >= lo * tiles) & (j < hi * tiles)

    def start(j, slot):
        use_far = between(j, 3, 4) | between(j, 5, 8)
        t = lax.rem(j, tiles)

        @pl.when(jnp.logical_not(use_far))
        def _():
            for c in tile_copies((wg0, wu0, wd0), t, slot):
                c.start()

        @pl.when(use_far)
        def _():
            for c in tile_copies((wg1, wu1, wd1), t, slot):
                c.start()

    def x_copy(src, slot):
        return pltpu.make_async_copy(src, xbuf.at[slot], sem_x.at[slot])

    acc[...] = jnp.zeros_like(acc)
    x_sources = (xa_hbm, xb_hbm, in_a, in_b, xa_hbm, xb_hbm)
    chunk = ROW_BLOCK // 2

    def chunks(fn):
        @pl.loop(0, m // chunk)
        def _(i):
            fn(pl.ds(pl.multiple_of(i * chunk, chunk), chunk))

    def body(j, carry):
        slot = lax.rem(j, 2)

        @pl.when(j == 2 * tiles - 4)
        def _():
            rows[1].start()

        @pl.when(j == 3 * tiles - 2)
        def _():
            for c in far:
                c.wait_recv()

        for k in range(1, 6):
            @pl.when(j == starts[k] - 2)
            def _():
                if k in (2, 3):
                    rows[k - 2].wait_recv()
                x_copy(x_sources[k], k % 2).start()

        for k in (4, 5):
            @pl.when(j == starts[k] + tiles - 3)
            def _():
                pltpu.make_async_copy((mid_a, mid_b)[k - 4], mid, sem_in.at[0]).start()

        for k in (2, 3):
            @pl.when(j == starts[k + 1] + 1)
            def _():
                pltpu.make_async_copy(stage, (send_a, send_b)[k - 2], sem_out.at[0]).wait()
                rows[k].start()

        for k in range(6):
            @pl.when(j == starts[k])
            def _():
                x_copy(x_sources[k], k % 2).wait()

        @pl.when(j + 1 < steps)
        def _():
            start(j + 1, 1 - slot)

        for c in tile_copies((wg0, wu0, wd0), 0, slot):
            c.wait()

        first = j == starts[0]
        odd = jnp.int32(0)
        for k in range(1, 6):
            first = first | (j == starts[k])
            odd = odd + (j >= starts[k]).astype(jnp.int32)
        odd = lax.rem(odd, 2)
        acts = []
        for r in range(0, m, ROW_BLOCK):
            x = xbuf[odd, r:r + ROW_BLOCK]
            g = fdot(x, gb[slot])
            u = fdot(x, ub[slot])
            t = jnp.tanh(g * (GELU_A + GELU_B * (g * g)))
            acts.append((g * (0.5 + 0.5 * t) * u).astype(jnp.bfloat16))
        for i, r in enumerate(range(0, m, ROW_BLOCK)):
            acc[r:r + ROW_BLOCK] = jnp.where(first, 0.0, acc[r:r + ROW_BLOCK]) + fdot(acts[i], db[slot])

        for k in (0, 1):
            @pl.when(j == starts[k + 1] - 1)
            def _():
                def keep(sl):
                    own[k, sl] = acc[sl].astype(jnp.bfloat16)

                chunks(keep)

        for k in (2, 3):
            @pl.when(j == starts[k + 1] - 1)
            def _():
                def put(sl):
                    stage[sl] = acc[sl].astype(jnp.bfloat16)

                chunks(put)
                pltpu.make_async_copy(stage, (send_a, send_b)[k - 2], sem_out.at[0]).start()

        for k in (4, 5):
            @pl.when(j == starts[k] + tiles - 1)
            def _():
                ret, mid_k = ((ret_a, mid_a), (ret_b, mid_b))[k - 4]
                rows[k - 2].wait_recv()
                got = pltpu.make_async_copy(ret, their, sem_in.at[1])
                got.start()
                pltpu.make_async_copy(mid_k, mid, sem_in.at[0]).wait()
                got.wait()
                if k == 5:
                    pltpu.make_async_copy(stage, out_hbm.at[pl.ds(0, m)], sem_out.at[1]).wait()

                def finish(sl):
                    total = acc[sl] + own[k - 4, sl].astype(jnp.float32) + their[sl].astype(jnp.float32)
                    stage[sl] = (mid[sl].astype(jnp.float32) + total.astype(jnp.bfloat16).astype(jnp.float32)).astype(jnp.bfloat16)

                chunks(finish)
                pltpu.make_async_copy(stage, out_hbm.at[pl.ds((k - 4) * m, m)], sem_out.at[k - 3]).start()
        return carry

    lax.fori_loop(0, steps, body, 0)
    pltpu.make_async_copy(stage, out_hbm.at[pl.ds(m, m)], sem_out.at[2]).wait()
    for c in rows + far:
        c.wait_send()


def mlp_call(x, mid, weights):
    m, d = x.shape[0] // 2, x.shape[1]
    f = weights[0].shape[1]
    half = jax.ShapeDtypeStruct((m, d), jnp.bfloat16)
    outs = [jax.ShapeDtypeStruct((2 * m, d), jnp.bfloat16)] + [jax.ShapeDtypeStruct(w.shape, w.dtype) for w in weights] + [half] * 6
    dma = pltpu.SemaphoreType.DMA
    return pl.pallas_call(
        mlp_kernel,
        in_specs=[ANY] * 5,
        out_specs=[ANY] * len(outs),
        out_shape=outs,
        scratch_shapes=[
            pltpu.VMEM((2, m, d), jnp.bfloat16), pltpu.VMEM((2, m, d), jnp.bfloat16), pltpu.VMEM((m, d), jnp.float32),
            pltpu.VMEM((m, d), jnp.bfloat16), pltpu.VMEM((m, d), jnp.bfloat16), pltpu.VMEM((m, d), jnp.bfloat16),
            pltpu.VMEM((2, d, F_TILE), jnp.bfloat16), pltpu.VMEM((2, d, F_TILE), jnp.bfloat16), pltpu.VMEM((2, F_TILE, d), jnp.bfloat16),
            dma((2, 3)), dma((2,)), dma((2,)), dma((3,)), dma((3,)), dma((3,)), dma((4,)), dma((4,)),
        ],
        compiler_params=params(60, collective_id=0, has_side_effects=True),
        cost_estimate=cost(48 * m * d * f, 48 * d * f),
        name="mlp",
    )(x, mid, *weights)[0]


def copy_kernel(src_ref, dst_ref):
    dst_ref[...] = src_ref[...]


def copy_call(a):
    blk = pl.BlockSpec((ROW_BLOCK // 2, a.shape[1]), lambda i: (i, 0))
    return pl.pallas_call(
        copy_kernel,
        grid=(2 * a.shape[0] // ROW_BLOCK,),
        in_specs=[blk],
        out_specs=blk,
        out_shape=jax.ShapeDtypeStruct(a.shape, a.dtype),
        compiler_params=params(60),
        cost_estimate=cost(a.size, 4 * a.size),
        name="result",
    )(a)


def solution(mesh):
    tp_size, dp_size = mesh.shape["tp"], mesh.shape["dp"]
    row_spec = P("dp", "tp", None)
    arg_specs = (row_spec, P("dp"), P("dp"), P(), P(None, "tp"), P(), P(), P("tp", None), P(), P(None, "tp"), P(None, "tp"), P("tp", None))

    def swap(a, axis, bit):
        return lax.ppermute(a, axis, [(i, i ^ bit) for i in range(mesh.shape[axis])])

    def spread(w, me_dp):
        size = w.shape[0] // dp_size
        quarter = lax.dynamic_slice_in_dim(w, me_dp * size, size, axis=0)
        return swap(quarter, "tp", 2)

    def gather(got, diag_first):
        y = swap(got, "dp", 1)
        z = swap(got, "dp", 2)
        diag = swap(y, "dp", 2) if diag_first else swap(z, "dp", 1)
        far = [got, y, z, diag]
        return far + [swap(a, "tp", 1) for a in far]

    def local_layer(hidden, prefix_len, valid_len, norm_attn, w_query, w_key, w_value, w_out, norm_mlp, w_gate, w_up, w_down):
        nb, rows, d = hidden.shape
        head_dim = w_key.shape[1]
        half = nb // 2
        me, me_dp = lax.axis_index("tp"), lax.axis_index("dp")
        group = jnp.bitwise_xor(me_dp, jnp.arange(dp_size, dtype=jnp.int32))
        pos = jnp.bitwise_xor(me, jnp.arange(tp_size, dtype=jnp.int32)) * rows
        cos, sin = rope_tables(me * rows + jnp.arange(rows), head_dim)

        wq_got = spread(w_query, me_dp)
        wo_got = spread(w_out, me_dp)
        w_query_c = swap(w_query, "tp", 1)
        normed, key_local, value_local, kv_a, kv_b = kv_call(hidden, norm_attn[None], w_key, w_value, cos, sin)
        kvs = []
        for kv in (kv_a, kv_b):
            kv_x = swap(kv, "tp", 2)
            kvs.append((kv, swap(kv, "tp", 1), kv_x, swap(kv_x, "tp", 1)))
        query_a = query_call(normed, (w_query, w_query_c), cos, sin, head_dim)
        query_b = query_call(normed, gather(wq_got, True), cos, sin, head_dim, group)
        w_outs = [w_out, swap(w_out, "tp", 1)] + gather(wo_got, False)
        near = (w_gate, w_up, w_down)

        o = None
        for base, kv in ((0, kvs[0]), (half, kvs[1])):
            o = attn_call(base, half, pos, prefix_len, valid_len, query_a, query_b, kv, o)
        mid, x = out_call(0, o, hidden, group, w_outs, norm_mlp[None])
        out = copy_call(mlp_call(x, mid, near))
        return out.reshape(nb, rows, d), key_local, value_local

    return jax.shard_map(local_layer, mesh=mesh, in_specs=arg_specs, out_specs=(row_spec, row_spec, row_spec), check_vma=False)
```
